256 devices in a mesh: expert: 32 (over z, x_lo, core), tensor: 8 (over y, x_hi).
Axes of the slice: x: 4 (x_hi: 2, x_lo: 2; x = x_hi * 2 + x_lo), y: 4, z: 8, core: 2. Of those that a mesh axis runs over, the one named last changes fastest.
Arguments:
- tokens: bfloat16 [2048, 2048], P('expert'), may hold values from -6 to 6
- expert_ids: int32 [2048, 6], replicated, may hold values from 0 to 63, all different within a row; in each aligned block of 2048 rows (0 to 2047, 2048 to 4095, ...) at most 256 rows name the same one
- gate_probs: float32 [2048, 6], replicated, may hold values from 0.02 to 0.6
- w_gate: bfloat16 [64, 2048, 1408], P('expert', None, 'tensor'), may hold values from -0.125 to 0.125
- w_up: bfloat16 [64, 2048, 1408], P('expert', None, 'tensor'), may hold values from -0.125 to 0.125
- w_down: bfloat16 [64, 1408, 2048], P('expert', 'tensor'), may hold values from -0.15625 to 0.15625
- shared_gate: bfloat16 [2048, 2816], P(None, 'tensor'), may hold values from -0.125 to 0.125
- shared_up: bfloat16 [2048, 2816], P(None, 'tensor'), may hold values from -0.125 to 0.125
- shared_down: bfloat16 [2816, 2048], P('tensor'), may hold values from -0.109375 to 0.109375
Outputs:
- layer_out: bfloat16 [2048, 2048], P('expert')
The draws below stay inside these ranges and needn't reach their ends.
Inputs may be any that keep to these rules, and one draw needn't show every extreme that they name: `expert_ids`: each row names 6 different experts. Over all 2048 tokens no expert is named more than 256 times, a bound that some block reaches.
All inputs are finite; a program needn't handle non-finite values.
Results may differ from the reference program's by a relative error of at most 0.011.
Values may be sent and summed in bfloat16 or wider, within the bound.
A program may use at most 64 MiB of HBM per device.

```python
import math
import jax
import jax.numpy as jnp
import numpy as np
from jax import lax

D = 2048
RF = 1408
SF = 2816
TOPK = 6
EXPERTS = 64
TOKENS = 2048
CAP = 256


def levels(rng, extent, cuts, least, top_value):
    def one(axis_at, shards_of):
        steps = jax.random.uniform(jax.random.fold_in(jax.random.fold_in(rng, 6), axis_at), (shards_of,), jnp.float32, least / len(cuts), top_value / len(cuts))
        return jnp.repeat(jnp.exp(steps), extent[axis_at] // shards_of).reshape((-1,) + (1,) * (len(extent) - axis_at - 1))

    loudness = one(*cuts[0])
    for cut in cuts[1:]:
        loudness = loudness * one(*cut)
    return loudness


def assign_block(rng, own, number, rows, amount, top, bound, slope):
    ranking = jax.random.permutation(rng, amount)
    packed, common = shares(amount, rows * top, bound, slope, True), shares(amount, rows * top, bound, slope, False)
    places = jnp.arange(amount)

    def named(lengths, rotation):
        used = int((lengths > 0).sum())
        fixed = max(1, used // 4)
        shifted = fixed + (places - fixed + rotation * (used - fixed)) % max(1, amount - fixed)
        return jnp.zeros((amount,), jnp.int32).at[ranking[jnp.where(places < fixed, places, shifted)]].set(jnp.asarray(lengths, jnp.int32))

    lengths = jnp.where(number % 4 == 0, named(packed, number // 4), named(common, number - number // 4 - 1))
    mixed = jax.random.permutation(jax.random.fold_in(own, 3), amount)
    source_of, taker = mixed[0:amount // 2 * 2:2], mixed[1:amount // 2 * 2:2]
    margin = jnp.minimum(lengths[source_of] - 1, bound - lengths[taker]) // 2
    margin = jnp.where((source_of == ranking[0]) | (taker == ranking[0]) | (lengths[taker] == 0), 0, jnp.maximum(margin, 0))
    shifted = jax.random.randint(jax.random.fold_in(own, 4), (amount // 2,), 0, 1 << 20) % (margin + 1)
    lengths = lengths.at[source_of].add(-shifted).at[taker].add(shifted)
    labels = jnp.searchsorted(jnp.cumsum(lengths), jnp.arange(rows * top), side="right").astype(jnp.int32)
    grid = labels.reshape(top, rows).T
    grid = grid[jax.random.permutation(jax.random.fold_in(own, 1), rows)]
    rotation = jax.random.randint(jax.random.fold_in(own, 2), (rows, 1), 0, top)
    return jnp.take_along_axis(grid, (jnp.arange(top)[None, :] + rotation) % top, axis=1)


def shares(number_of, total, most, skew, full):
    weights = [(1 << 20) // math.isqrt(grade ** skew) + 1 for grade in range(1, number_of + 1)]
    largest = most if full else min(most, max(-(-total // number_of), total * weights[0] // sum(weights)))
    least = 1 if total - largest >= number_of - 1 else 0
    holding, rest = [largest] + [least] * (number_of - 1), total - largest - least * (number_of - 1)
    while rest > 0:
        free = [i for i in range(1, number_of) if holding[i] < largest] or [i for i in range(1, number_of) if holding[i] < most]
        mass, budget = sum([weights[i] for i in free]), rest
        for i in free:
            addition = min(most - holding[i], max(1, budget * weights[i] // mass), rest)
            holding[i] = holding[i] + addition
            rest = rest - addition
    return np.array(holding)


def bell_draw(own_key, shape, scale, bound, split=(), kind=jnp.bfloat16):
    entries = scale * jax.random.normal(own_key, shape, jnp.float32)
    if split:
        entries = entries * levels(own_key, shape, split, -0.22, 0.18)
    return jnp.clip(entries, -bound, bound).astype(kind)


def setup_inputs(seed: int = 0) -> dict:
    arg_keys = jax.random.split(jax.random.key(seed), 10)
    tokens = bell_draw(arg_keys[0], (TOKENS, D), 1.0, 6.0, ((0, 32),))
    expert_ids_keys = jax.random.split(jax.random.fold_in(arg_keys[1], 1), TOKENS // TOKENS)
    expert_ids_turns = jax.random.permutation(jax.random.fold_in(arg_keys[1], 3), TOKENS // TOKENS)
    expert_ids = jax.vmap(lambda own, number: assign_block(jax.random.fold_in(arg_keys[1], 2), own, number, TOKENS, EXPERTS, TOPK, CAP, 2))(expert_ids_keys, expert_ids_turns).reshape((TOKENS, TOPK))
    gate_probs = jnp.clip(jnp.exp(jax.random.uniform(arg_keys[2], (TOKENS, TOPK), jnp.float32, math.log(0.02), math.log(0.6))), 0.02, 0.6)
    w_gate = bell_draw(arg_keys[3], (EXPERTS, D, RF), D ** -0.5, 0.125, ((0, 32), (2, 8)))
    w_up = bell_draw(arg_keys[4], (EXPERTS, D, RF), D ** -0.5, 0.125, ((0, 32), (2, 8)))
    w_down = bell_draw(arg_keys[5], (EXPERTS, RF, D), RF ** -0.5, 0.15625, ((0, 32), (1, 8)))
    shared_gate = bell_draw(arg_keys[6], (D, SF), D ** -0.5, 0.125, ((1, 8),))
    shared_up = bell_draw(arg_keys[7], (D, SF), D ** -0.5, 0.125, ((1, 8),))
    shared_down = bell_draw(arg_keys[8], (SF, D), SF ** -0.5, 0.109375, ((0, 8),))
    return {"tokens": tokens, "expert_ids": expert_ids, "gate_probs": gate_probs, "w_gate": w_gate, "w_up": w_up, "w_down": w_down, "shared_gate": shared_gate, "shared_up": shared_up, "shared_down": shared_down}


def reference(tokens, expert_ids, gate_probs, w_gate, w_up, w_down, shared_gate, shared_up, shared_down):
    flat_ids = expert_ids.reshape(-1)
    onehot = (flat_ids[:, None] == jnp.arange(EXPERTS, dtype=jnp.int32)[None, :]).astype(jnp.int32)
    before = jnp.cumsum(onehot, axis=0) - onehot
    slot = jnp.sum(before * onehot, axis=1).reshape(expert_ids.shape).astype(jnp.int32)
    positions = jnp.arange(CAP, dtype=jnp.int32)

    def one_expert(total, inputs):
        gate_w, up_w, down_w, expert = inputs
        hits = expert_ids == expert
        target = jnp.sum(jnp.where(hits, slot + 1, 0), axis=1) - 1
        weight = jnp.sum(jnp.where(hits, gate_probs, 0.0), axis=1)
        picker = (positions[:, None] == target[None, :]).astype(jnp.bfloat16)
        dispatched = jnp.dot(picker, tokens, preferred_element_type=jnp.float32).astype(jnp.bfloat16)
        gate = jnp.dot(dispatched, gate_w, preferred_element_type=jnp.float32)
        upper = jnp.dot(dispatched, up_w, preferred_element_type=jnp.float32)
        hidden = (jax.nn.silu(gate) * upper).astype(jnp.bfloat16)
        slot_out = jnp.dot(hidden, down_w, preferred_element_type=jnp.float32)
        back = jnp.dot(picker.astype(jnp.float32).T, slot_out, precision=lax.Precision.HIGHEST)
        return total + weight[:, None] * back, None

    start = jnp.zeros(tokens.shape, jnp.float32)
    routed, _ = lax.scan(one_expert, start, (w_gate, w_up, w_down, jnp.arange(EXPERTS, dtype=jnp.int32)))
    sgate = jnp.dot(tokens, shared_gate, preferred_element_type=jnp.float32)
    supper = jnp.dot(tokens, shared_up, preferred_element_type=jnp.float32)
    shared_hidden = (jax.nn.silu(sgate) * supper).astype(jnp.bfloat16)
    shared = jnp.dot(shared_hidden, shared_down, preferred_element_type=jnp.float32)
    return (shared + routed).astype(jnp.bfloat16)
```

```python
import jax
import jax.numpy as jnp
from jax import lax
from jax.experimental import pallas as pl
from jax.experimental.pallas import tpu as pltpu
from jax.sharding import Mesh
from jax.sharding import PartitionSpec as P

MESH = pl.DeviceIdType.MESH
NZ, NT = 8, 8
OFFSETS = (0, -1, 1, -2, 2, -3, 3, 4)
SLOT = {d % NZ: s for s, d in enumerate(OFFSETS)}
BF, F32 = jnp.bfloat16, jnp.float32
NT_DIMS = (((1,), (1,)), ((), ()))


def kernel(
    tokens, ids, probs, wg, wu, wd, sg, su, sd, out,
    gath, part, dd, xx, zin, zout, wgv, wuv, wdv, sgv, suv, sdv, idv, prv, hbuf, sbuf,
    tsb, tsi, fin, agi,
    loc_sem, snd_sem, ag_sem, dd_sem, xx_sem, zin_sem, ts_sem, ta_sem,
):
    z, xl, c = lax.axis_index("z"), lax.axis_index("xl"), lax.axis_index("c")
    y, xh = lax.axis_index("y"), lax.axis_index("xh")
    t = y * 2 + xh
    rows = tokens.shape[0]
    half = rows // 2
    width = wg.shape[0] // 2
    group = 4 * rows
    zup, zdn = {"z": lax.rem(z + 1, NZ)}, {"z": lax.rem(z + NZ - 1, NZ)}
    xup = {"xl": 1 - xl, "xh": lax.rem(xh + xl, 2)}
    xdn = {"xl": 1 - xl, "xh": lax.rem(xh + 1 - xl, 2)}
    mate = {"c": 1 - c}
    peers = []
    for i in range(1, NT):
        tp = lax.rem(t + i, NT)
        peers.append((tp, {"y": tp // 2, "xh": lax.rem(tp, 2)}))

    local = []

    def load(src, dst):
        cp = pltpu.make_async_copy(src, dst, loc_sem.at[len(local)])
        cp.start()
        local.append(cp)
        return cp

    own = xl * 2 + c
    tok_cp = load(tokens, gath.at[0, own])
    sh_cp = [load(sg, sgv), load(su, suv), load(sd, sdv)]
    rt_cp = [load(ids, idv), load(probs, prv), load(wg, wgv), load(wu, wuv), load(wd, wdv)]

    barrier = pltpu.get_barrier_semaphore()
    greeted = [zup, zdn, xup, xdn, mate] + [p for _, p in peers]
    for dev in greeted:
        pl.semaphore_signal(barrier, inc=1, device_id=dev, device_id_type=MESH)
    pl.semaphore_wait(barrier, len(greeted))

    sent = []

    def send(src, dst, sem, dev):
        cp = pltpu.make_async_remote_copy(
            src_ref=src, dst_ref=dst, send_sem=snd_sem.at[len(sent)], recv_sem=sem,
            device_id=dev, device_id_type=MESH,
        )
        cp.start()
        sent.append(cp)

    def arrive(dst, sem):
        pltpu.make_async_remote_copy(
            src_ref=dst, dst_ref=dst, send_sem=snd_sem.at[0], recv_sem=sem,
            device_id=mate, device_id_type=MESH,
        ).wait_recv()

    def unit(slot, b, h):
        return gath.at[slot, b, pl.ds(h * half, half)]

    def spread(slot, b, h, from_z=True):
        ref, sem = unit(slot, b, h), ag_sem.at[slot, b, h]
        if from_z:
            send(ref, ref, sem, xup if h == 0 else xdn)
        send(ref, ref, sem, mate)

    def hop(offset, h, up):
        nxt = SLOT[(offset - 1 if up else offset + 1) % NZ]
        send(unit(SLOT[offset % NZ], own, h), unit(nxt, own, h), ag_sem.at[nxt, own, h], zup if up else zdn)

    def slots(k):
        return (0,) if k == 0 else (7,) if k == 4 else (2 * k - 1, 2 * k)

    def gather_z(k):
        for h in (0, 1):
            for up in (True, False):
                if k == 4 and up != (h == 0):
                    continue
                offset = -k if up else k
                slot = SLOT[offset % NZ]
                arrive(unit(slot, own, h), ag_sem.at[slot, own, h])
                if k < 3 or (k == 3 and up == (h == 0)):
                    hop(offset, h, up)
                spread(slot, own, h)

    def gather_x(k):
        b = (1 - xl) * 2 + c
        for h in (0, 1):
            for slot in slots(k):
                arrive(unit(slot, b, h), ag_sem.at[slot, b, h])
                spread(slot, b, h, from_z=False)

    def gather_mate(k):
        for slot in slots(k):
            for a in (0, 1):
                b = a * 2 + 1 - c
                for h in (0, 1):
                    arrive(unit(slot, b, h), ag_sem.at[slot, b, h])

    def ffn(x, g_ref, u_ref, d_ref, scale, write):
        m = x.shape[0]
        g = lax.dot_general(x, g_ref[...], NT_DIMS, preferred_element_type=F32)
        u = lax.dot_general(x, u_ref[...], NT_DIMS, preferred_element_type=F32)
        h = g / (1.0 + jnp.exp(-g)) * u
        if scale is not None:
            h = h * scale
        hbuf[pl.ds(0, m), :] = h.astype(BF)

        @pl.loop(0, 4)
        def _(n):
            cols = pl.ds(pl.multiple_of(n * 512, 512), 512)
            write(cols, jnp.dot(hbuf[pl.ds(0, m), :], d_ref[:, cols], preferred_element_type=F32))

    def column(slot, expert):
        gz = lax.rem(z + OFFSETS[slot] + NZ, NZ)
        lanes = pl.ds(pl.multiple_of(gz * group, group), group)
        row = jnp.sum(jnp.where(idv[:, lanes] == expert, prv[:, lanes], 0.0), axis=0, keepdims=True)
        return jnp.broadcast_to(row, (128, group)).T[:, :1]

    def compute(k):
        ss = slots(k)
        s0, ns = ss[0], len(ss)
        m = ns * group
        first = (z * 4 + xl * 2 + c) * 2
        w0, w1 = (
            jnp.concatenate([column(s, first + j) for s in ss], axis=0) for j in (0, 1)
        )
        lane = lax.broadcasted_iota(jnp.int32, (m, 2 * width), 1)
        scale = jnp.where(lane < width, w0, w1)

        def write(cols, p):
            part[pl.ds(s0, ns), :, :, cols] = p.astype(BF).reshape(ns, 4, rows, 512)

        ffn(gath[pl.ds(s0, ns)].reshape(m, gath.shape[-1]), wgv, wuv, wdv, scale, write)

    def swap_mate(k):
        for slot in slots(k):
            for a in (1 - xl, xl):
                send(part.at[slot, a * 2 + 1 - c], dd.at[slot, a], dd_sem.at[slot, a], mate)

    def swap_x(k):
        a = 1 - xl
        b = a * 2 + c
        for slot in slots(k):
            arrive(dd.at[slot, a], dd_sem.at[slot, a])
            part[slot, b] = (part[slot, b].astype(F32) + dd[slot, a].astype(F32)).astype(BF)
            for h, dev in ((0, xup), (1, xdn)):
                r = pl.ds(h * half, half)
                send(part.at[slot, b, r], xx.at[slot, r], xx_sem.at[slot, h], dev)

    seen = set()

    def ring_term(slot, h):
        if slot not in seen:
            seen.add(slot)
            arrive(dd.at[slot, xl], dd_sem.at[slot, xl])
        r = pl.ds(h * half, half)
        arrive(xx.at[slot, r], xx_sem.at[slot, h])
        return part[slot, own, r].astype(F32) + dd[slot, xl, r].astype(F32) + xx[slot, r].astype(F32)

    quarter = half // 2

    def ring(s):
        terms = [ring_term(SLOT[(-s if up else s) % NZ], h) for h, up in ((0, True), (1, False))]
        for q in (0, 1):
            r = pl.ds(q * quarter, quarter)
            for h, up in ((0, True), (1, False)):
                acc = terms[h][q * quarter : (q + 1) * quarter]
                if s > 1:
                    arrive(zin.at[h, s - 2, r], zin_sem.at[h, s - 2, q])
                    acc = acc + zin[h, s - 2, r].astype(F32)
                zout[h, s - 1, r] = acc.astype(BF)
                send(zout.at[h, s - 1, r], zin.at[h, s - 1, r], zin_sem.at[h, s - 1, q], zup if up else zdn)

    tok_cp.wait()
    for h in (0, 1):
        hop(0, h, True)
        hop(0, h, False)
        spread(0, own, h)

    for cp in sh_cp:
        cp.wait()

    def write_shared(cols, p):
        sbuf[:, cols] = p

    ffn(gath[0, own], sgv, suv, sdv, None, write_shared)
    for cp in rt_cp:
        cp.wait()
    gather_x(0)
    gather_mate(0)
    gather_z(1)
    compute(0)
    gather_x(1)
    gather_z(2)
    gather_mate(1)
    compute(1)
    swap_mate(1)
    gather_x(2)
    gather_z(3)
    swap_x(1)
    gather_mate(2)
    compute(2)
    swap_mate(2)
    gather_x(3)
    gather_z(4)
    ring(1)
    swap_x(2)
    gather_x(4)
    gather_mate(3)
    compute(3)
    swap_mate(3)
    ring(2)
    swap_x(3)
    gather_mate(4)
    compute(4)
    swap_mate(4)
    ring(3)
    swap_x(4)
    swap_mate(0)
    ring(4)
    swap_x(0)
    ring(5)
    ring(6)
    ring(7)
    for h in (0, 1):
        r = pl.ds(h * half, half)
        acc = ring_term(0, h) + sbuf[r, :]
        for q in (0, 1):
            rq = pl.ds(q * quarter, quarter)
            arrive(zin.at[h, NZ - 2, rq], zin_sem.at[h, NZ - 2, q])
        acc = (acc + zin[h, NZ - 2].astype(F32)).astype(BF)
        for i in range(NT):
            tsb[i, r, :] = acc[:, i * 256 : (i + 1) * 256]
    for tp, dev in peers:
        send(tsb.at[tp], tsi.at[t], ts_sem.at[t], dev)
    acc = tsb[t].astype(F32)
    for tp, _ in peers:
        arrive(tsi.at[tp], ts_sem.at[tp])
        acc = acc + tsi[tp].astype(F32)
    fin[...] = acc.astype(BF)
    for tp, dev in peers:
        send(fin, agi.at[t], ta_sem.at[t], dev)
    agi[t] = fin[...]
    for tp, _ in peers:
        arrive(agi.at[tp], ta_sem.at[tp])
    for i in range(NT):
        out[:, i * 256 : (i + 1) * 256] = agi[i]
    for cp in sent:
        cp.wait_send()


def layer(tokens, ids, probs, wg, wu, wd, sg, su, sd):
    rows, dim = tokens.shape
    hid = sg.shape[0]
    any_spec = pl.BlockSpec(memory_space=pl.ANY)
    wide = pltpu.VMEM((hid, dim), BF)
    dma = pltpu.SemaphoreType.DMA
    return pl.pallas_call(
        kernel,
        out_shape=jax.ShapeDtypeStruct((rows, dim), BF),
        in_specs=[any_spec] * 9,
        out_specs=pl.BlockSpec(memory_space=pltpu.VMEM),
        scratch_shapes=[
            pltpu.VMEM((NZ, 4, rows, dim), BF),
            pltpu.VMEM((NZ, 4, rows, dim), BF),
            pltpu.VMEM((NZ, 2, rows, dim), BF),
            pltpu.VMEM((NZ, rows, dim), BF),
            pltpu.VMEM((2, NZ - 1, rows // 2, dim), BF),
            pltpu.VMEM((2, NZ - 1, rows // 2, dim), BF),
            wide, wide, wide, wide, wide, wide,
            pltpu.VMEM(ids.shape, jnp.int32),
            pltpu.VMEM(probs.shape, F32),
            pltpu.VMEM((8 * rows, hid), BF),
            pltpu.VMEM((rows, dim), F32),
            pltpu.VMEM((NT, rows, dim // NT), BF),
            pltpu.VMEM((NT, rows, dim // NT), BF),
            pltpu.VMEM((rows, dim // NT), BF),
            pltpu.VMEM((NT, rows, dim // NT), BF),
            dma((9,)), dma((160,)), dma((NZ, 4, 2)), dma((NZ, 2)), dma((NZ, 2)),
            dma((2, NZ - 1, 2)), dma((NT,)), dma((NT,)),
        ],
        compiler_params=pltpu.CompilerParams(
            collective_id=0, has_side_effects=True, vmem_limit_bytes=60 * 1024 * 1024
        ),
    )(tokens, ids, probs, wg, wu, wd, sg, su, sd)


def body(tokens, expert_ids, gate_probs, w_gate, w_up, w_down, shared_gate, shared_up, shared_down):
    dim = tokens.shape[1]
    stacked = lambda w: jnp.swapaxes(w, 1, 2).reshape(-1, dim)
    return layer(
        tokens, expert_ids.T, gate_probs.T, stacked(w_gate), stacked(w_up), w_down.reshape(-1, dim),
        shared_gate.T, shared_up.T, shared_down,
    )


def solution(mesh):
    torus = Mesh(mesh.devices.reshape(NZ, 2, 2, 4, 2), ("z", "xl", "c", "y", "xh"))
    e, t = ("z", "xl", "c"), ("y", "xh")
    return jax.shard_map(
        body,
        mesh=torus,
        in_specs=(
            P(e, None), P(), P(),
            P(e, None, t), P(e, None, t), P(e, t, None),
            P(None, t), P(None, t), P(t, None),
        ),
        out_specs=P(e, None),
        check_vma=False,
    )
```

```python
import jax
import jax.numpy as jnp
from jax import lax
from jax.experimental import pallas as pl
from jax.experimental.pallas import tpu as pltpu
from jax.sharding import Mesh
from jax.sharding import PartitionSpec as P

MESH = pl.DeviceIdType.MESH
NZ, NY = 8, 4
OFFSETS = (0, -1, 1, -2, 2, -3, 3, 4)
SLOT = {d % NZ: s for s, d in enumerate(OFFSETS)}
BF, F32 = jnp.bfloat16, jnp.float32
GA, GR = 512, 512
NT_DIMS = (((1,), (1,)), ((), ()))


def kernel(
    tokens, ids, probs, wg, wu, wd, sg, su, sd, out,
    gath, part, dd, yy, xx, zin, zout, wguv, wdv, sguv, sdv, idv, prv, hbuf, sbuf,
    tsb, tsi, fin, agi,
    loc_sem, snd_sem, ag_sem, ya_sem, ma_sem, dd_sem, yr_sem, xx_sem, zin_sem, ts_sem, ta_sem,
):
    z, xl, c = lax.axis_index("z"), lax.axis_index("xl"), lax.axis_index("c")
    y, xh = lax.axis_index("y"), lax.axis_index("xh")
    rows, dim = tokens.shape
    half, quarter = rows // 2, rows // 4
    width = wg.shape[0] // 2
    group = 4 * rows
    sa, sr = GA // NY, GR // NY
    ca, cr = dim - GA, dim - GR
    aw, rw = ca + sa, cr + sr
    zup, zdn = {"z": lax.rem(z + 1, NZ)}, {"z": lax.rem(z + NZ - 1, NZ)}
    xup = {"xl": 1 - xl, "xh": lax.rem(xh + xl, 2)}
    xdn = {"xl": 1 - xl, "xh": lax.rem(xh + 1 - xl, 2)}
    mate = {"c": 1 - c}
    yat = [lax.rem(y + i, NY) for i in range(NY)]
    peers = [(yat[i], lax.rem(xh + j, 2), i, j) for i in range(NY) for j in (0, 1)][1:]

    local = []

    def load(src, dst):
        cp = pltpu.make_async_copy(src, dst, loc_sem.at[len(local)])
        cp.start()
        local.append(cp)
        return cp

    def load_turned(src, dst, common, size):
        cps = [load(src.at[:, pl.ds(0, common)], dst.at[:, pl.ds(0, common)])]
        for i in range(NY if size else 0):
            at = pl.multiple_of(common + yat[i] * size, 128)
            cps.append(load(src.at[:, pl.ds(at, size)], dst.at[:, pl.ds(common + i * size, size)]))
        return cps

    def load_pair(g, u, dst):
        hid = g.shape[0]
        tail = hid - 256
        cps = []
        for src, at, n, to in ((g, 0, 256, 0), (u, 0, 256, 256), (g, 256, tail, 512), (u, 256, tail, 640)):
            cps += load_turned(src.at[pl.ds(at, n)], dst.at[pl.ds(to, n)], ca, sa)
        return cps

    own, other = c * 2 + xl, c * 2 + 1 - xl
    mine, mates = pl.ds(c * 2, 2), pl.ds((1 - c) * 2, 2)
    tok_cp = load_turned(tokens, gath.at[0, own], ca, sa)
    sh_cp = load_pair(sg, su, sguv) + load_turned(sd, sdv, cr, sr)
    rt_cp = [load(ids, idv), load(probs, prv)] + load_pair(wg, wu, wguv) + load_turned(wd, wdv, cr, sr)

    barrier = pltpu.get_barrier_semaphore()
    greeted = [zup, zdn, xup, xdn, mate] + [{"y": yp, "xh": xp} for yp, xp, _, _ in peers]
    for dev in greeted:
        pl.semaphore_signal(barrier, inc=1, device_id=dev, device_id_type=MESH)
    pl.semaphore_wait(barrier, len(greeted))

    sent = []

    def send(src, dst, sem, dev):
        cp = pltpu.make_async_remote_copy(
            src_ref=src, dst_ref=dst, send_sem=snd_sem.at[len(sent)], recv_sem=sem,
            device_id=dev, device_id_type=MESH,
        )
        cp.start()
        sent.append(cp)

    def arrive(dst, sem):
        pltpu.make_async_remote_copy(
            src_ref=dst, dst_ref=dst, send_sem=snd_sem.at[0], recv_sem=sem,
            device_id=mate, device_id_type=MESH,
        ).wait_recv()

    def slots(k):
        return (0,) if k == 0 else (7,) if k == 4 else (2 * k - 1, 2 * k)

    def unit(slot, b, h):
        return gath.at[slot, b, pl.ds(h * half, half), pl.ds(0, aw)]

    def hop(offset, h, up):
        nxt = SLOT[(offset - 1 if up else offset + 1) % NZ]
        send(unit(SLOT[offset % NZ], own, h), unit(nxt, own, h), ag_sem.at[nxt, 0, h], zup if up else zdn)

    def across(slot, h):
        send(unit(slot, own, h), unit(slot, own, h), ag_sem.at[slot, 1, h], xup if h == 0 else xdn)

    def gather_z(k):
        for h in (0, 1):
            for up in (True, False):
                if k == 4 and up != (h == 0):
                    continue
                offset = -k if up else k
                slot = SLOT[offset % NZ]
                arrive(unit(slot, own, h), ag_sem.at[slot, 0, h])
                if k < 3 or (k == 3 and up == (h == 0)):
                    hop(offset, h, up)
                across(slot, h)

    def fresh(slot):
        return pl.ds(other, 1) if slot == 0 else mine

    def main(slot):
        return gath.at[slot, fresh(slot), :, pl.ds(0, aw)]

    def piece(slot, i):
        return gath.at[slot, fresh(slot), :, pl.ds(ca + i * sa, sa)]

    def rest(slot):
        return gath.at[slot, fresh(slot), :, pl.ds(aw, dim - aw)]

    def gather_x(k):
        for slot in slots(k):
            for h in (0, 1):
                arrive(unit(slot, other, h), ag_sem.at[slot, 1, h])
            for i in range(1, NY if GA else 1):
                send(piece(slot, 0), piece(slot, NY - i), ya_sem.at[slot, NY - i - 1], {"y": yat[i]})
            send(main(slot), main(slot), ma_sem.at[slot, 0], mate)

    def gather_y(k):
        for slot in slots(k) if GA else ():
            for i in range(1, NY):
                arrive(piece(slot, i), ya_sem.at[slot, i - 1])
            send(rest(slot), rest(slot), ma_sem.at[slot, 1], mate)

    def gather_mate(k):
        for slot in slots(k):
            if slot == 0:
                arrive(gath.at[0, (1 - c) * 2 + xl], ma_sem.at[NZ, 0])
            blocks = pl.ds((1 - c) * 2 + 1 - xl, 1) if slot == 0 else mates
            arrive(gath.at[slot, blocks, :, pl.ds(0, aw)], ma_sem.at[slot, 0])
            if GA:
                arrive(gath.at[slot, blocks, :, pl.ds(aw, dim - aw)], ma_sem.at[slot, 1])

    def ffn(x, gu_ref, d_ref, scale, write):
        m = x.shape[0]
        hid = d_ref.shape[0]
        gu = lax.dot_general(x, gu_ref[...], NT_DIMS, preferred_element_type=F32)
        for at, g, u in (
            (0, gu[:, 0:256], gu[:, 256:512]),
            (256, gu[:, 512 : hid + 256], gu[:, 640 : hid + 384]),
        ):
            h = g / (1.0 + jnp.exp(-g)) * u
            if scale is not None:
                h = h * scale(at, h.shape[1])
            hbuf[pl.ds(0, m), pl.ds(at, h.shape[1])] = h.astype(BF)

        @pl.loop(0, 4)
        def _(n):
            cols = pl.ds(pl.multiple_of(n * 512, 512), 512)
            write(cols, jnp.dot(hbuf[pl.ds(0, m), :], d_ref[:, cols], preferred_element_type=F32))

    def column(slot, expert):
        gz = lax.rem(z + OFFSETS[slot] + NZ, NZ)
        lanes = pl.ds(pl.multiple_of(gz * group, group), group)
        row = jnp.sum(jnp.where(idv[:, lanes] == expert, prv[:, lanes], 0.0), axis=0, keepdims=True)
        col = jnp.broadcast_to(row, (128, group)).T
        return [col[b * rows : (b + 1) * rows, :1] for b in (0, 2, 1, 3)]

    def compute(k):
        ss = slots(k)
        s0, ns = ss[0], len(ss)
        m = ns * group
        first = (z * 4 + xl * 2 + c) * 2
        w0, w1 = (
            jnp.concatenate([w for s in ss for w in column(s, first + j)], axis=0) for j in (0, 1)
        )

        def scale(at, n):
            lane = at + lax.broadcasted_iota(jnp.int32, (m, n), 1)
            return jnp.where(lane < width, w0, w1)

        def write(cols, p):
            part[pl.ds(s0, ns), :, :, cols] = p.astype(BF).reshape(ns, 4, rows, 512)

        ffn(gath[pl.ds(s0, ns)].reshape(m, dim), wguv, wdv, scale, write)
        if k == 0:
            part[0, own] = (part[0, own].astype(F32) + sbuf[...]).astype(BF)

    def swap_mate(k):
        for slot in slots(k):
            send(part.at[slot, mates], dd.at[slot], dd_sem.at[slot], mate)

    def swap_y(k):
        for slot in slots(k):
            arrive(dd.at[slot], dd_sem.at[slot])
            if GR:
                cols = pl.ds(rw, dim - rw)
                both = part[slot, mine, :, cols].astype(F32) + dd[slot, :, :, cols].astype(F32)
                part[slot, mine, :, cols] = both.astype(BF)
            for i in range(1, NY if GR else 1):
                send(
                    part.at[slot, mine, :, pl.ds(cr + i * sr, sr)], yy.at[slot, NY - i - 1],
                    yr_sem.at[slot, NY - i - 1], {"y": yat[i]},
                )

    def summed(slot, b, x, r):
        common = part[slot, b, r, 0:cr].astype(F32) + dd[slot, x, r, 0:cr].astype(F32)
        if not GR:
            return [common]
        own_slice = part[slot, b, r, cr:rw].astype(F32) + dd[slot, x, r, cr:rw].astype(F32)
        for i in range(NY - 1):
            own_slice = own_slice + yy[slot, i, x, r].astype(F32)
        return [common, own_slice]

    bounds = [(0, cr), (cr, rw)][: 2 if GR else 1]

    def swap_x(k):
        for slot in slots(k):
            for i in range(NY - 1 if GR else 0):
                arrive(yy.at[slot, i], yr_sem.at[slot, i])
            for h, dev in ((0, xup), (1, xdn)):
                r = pl.ds(h * half, half)
                for (lo, hi), v in zip(bounds, summed(slot, other, 1 - xl, r)):
                    part[slot, other, r, lo:hi] = v.astype(BF)
                send(
                    part.at[slot, other, r, pl.ds(0, rw)], xx.at[slot, r], xx_sem.at[slot, h], dev
                )

    def ring(s):
        for h, up in ((0, True), (1, False)):
            slot = SLOT[(-s if up else s) % NZ]
            r = pl.ds(h * half, half)
            arrive(xx.at[slot, r], xx_sem.at[slot, h])
        for q in (0, 1):
            r = pl.ds(q * quarter, quarter)
            for h, up in ((0, True), (1, False)):
                slot = SLOT[(-s if up else s) % NZ]
                full = pl.ds(h * half + q * quarter, quarter)
                if s > 1:
                    arrive(zin.at[h, s - 2, r], zin_sem.at[h, s - 2, q])
                for (lo, hi), v in zip(bounds, summed(slot, own, xl, full)):
                    v = v + xx[slot, full, lo:hi].astype(F32)
                    if s > 1:
                        v = v + zin[h, s - 2, r, lo:hi].astype(F32)
                    zout[h, s - 1, r, lo:hi] = v.astype(BF)
                send(zout.at[h, s - 1, r], zin.at[h, s - 1, r], zin_sem.at[h, s - 1, q], zup if up else zdn)

    for cp in tok_cp:
        cp.wait()
    for h in (0, 1):
        hop(0, h, True)
        hop(0, h, False)
        across(0, h)
    send(gath.at[0, own], gath.at[0, own], ma_sem.at[NZ, 0], mate)

    for cp in sh_cp:
        cp.wait()

    def write_shared(cols, p):
        sbuf[:, cols] = p

    ffn(gath[0, own], sguv, sdv, None, write_shared)
    for cp in rt_cp:
        cp.wait()
    gather_z(1)
    gather_x(0)
    gather_y(0)
    gather_z(2)
    gather_x(1)
    gather_mate(0)
    compute(0)
    gather_y(1)
    gather_z(3)
    gather_x(2)
    gather_mate(1)
    compute(1)
    swap_mate(1)
    gather_y(2)
    gather_z(4)
    gather_x(3)
    swap_y(1)
    gather_mate(2)
    compute(2)
    swap_mate(2)
    gather_y(3)
    gather_x(4)
    swap_x(1)
    swap_y(2)
    gather_mate(3)
    compute(3)
    swap_mate(3)
    gather_y(4)
    ring(1)
    swap_x(2)
    swap_y(3)
    gather_mate(4)
    compute(4)
    swap_mate(4)
    swap_mate(0)
    ring(2)
    swap_x(3)
    swap_y(4)
    swap_y(0)
    ring(3)
    swap_x(4)
    swap_x(0)
    ring(4)
    ring(5)
    ring(6)
    ring(7)
    cw = cr // NY
    for h in (0, 1):
        r = pl.ds(h * half, half)
        arrive(xx.at[0, r], xx_sem.at[0, h])
        for q in (0, 1):
            rq = pl.ds(q * quarter, quarter)
            arrive(zin.at[h, NZ - 2, rq], zin_sem.at[h, NZ - 2, q])
        for (lo, hi), v in zip(bounds, summed(0, own, xl, r)):
            v = (v + xx[0, r, lo:hi].astype(F32) + zin[h, NZ - 2, :, lo:hi].astype(F32)).astype(BF)
            if lo == 0:
                for i in range(NY):
                    tsb[i, h, :, 0:cw] = v[:, i * cw : (i + 1) * cw]
            else:
                tsb[y, h, :, cw : cw + sr] = v
    for yp, xp, i, j in peers:
        n = cw + sr if i == 0 else cw
        send(
            tsb.at[yp, xp, :, pl.ds(0, n)], tsi.at[(NY - i) % NY, j, :, pl.ds(0, n)],
            ts_sem.at[(NY - i) % NY, j], {"y": yp, "xh": xp},
        )
    acc = tsb[y, xh, :, 0:cw].astype(F32)
    for _, _, i, j in peers:
        n = cw + sr if i == 0 else cw
        arrive(tsi.at[i, j, :, pl.ds(0, n)], ts_sem.at[i, j])
        acc = acc + tsi[i, j, :, 0:cw].astype(F32)
    fin[:, 0:cw] = acc.astype(BF)
    if GR:
        fin[:, cw : cw + sr] = (
            tsb[y, xh, :, cw : cw + sr].astype(F32) + tsi[0, 1, :, cw : cw + sr].astype(F32)
        ).astype(BF)
    for yp, xp, i, j in peers:
        send(fin, agi.at[y, xh], ta_sem.at[(NY - i) % NY, j], {"y": yp, "xh": xp})
    agi[y, xh] = fin[...]
    for yp, xp, i, j in peers:
        arrive(agi.at[yp, xp], ta_sem.at[i, j])
    for i in range(NY):
        for j in (0, 1):
            r = pl.ds(j * half, half)
            out[r, i * cw : (i + 1) * cw] = agi[i, j, :, 0:cw]
            if GR:
                out[r, cr + i * sr : cr + (i + 1) * sr] = agi[i, j, :, cw : cw + sr]
    for cp in sent:
        cp.wait_send()


def layer(tokens, ids, probs, wg, wu, wd, sg, su, sd):
    rows, dim = tokens.shape
    hid = sg.shape[0]
    rw = dim - GR + GR // NY
    any_spec = pl.BlockSpec(memory_space=pl.ANY)
    pair, down = pltpu.VMEM((hid + 384, dim), BF), pltpu.VMEM((hid, dim), BF)
    dma = pltpu.SemaphoreType.DMA
    last = (NY, 2, rows // 2, dim // NY)
    return pl.pallas_call(
        kernel,
        out_shape=jax.ShapeDtypeStruct((rows, dim), BF),
        in_specs=[any_spec] * 9,
        out_specs=pl.BlockSpec(memory_space=pltpu.VMEM),
        scratch_shapes=[
            pltpu.VMEM((NZ, 4, rows, dim), BF),
            pltpu.VMEM((NZ, 4, rows, dim), BF),
            pltpu.VMEM((NZ, 2, rows, dim), BF),
            pltpu.VMEM((NZ, NY - 1, 2, rows, max(GR // NY, 128)), BF),
            pltpu.VMEM((NZ, rows, rw), BF),
            pltpu.VMEM((2, NZ - 1, rows // 2, rw), BF),
            pltpu.VMEM((2, NZ - 1, rows // 2, rw), BF),
            pair, down, pair, down,
            pltpu.VMEM(ids.shape, jnp.int32),
            pltpu.VMEM(probs.shape, F32),
            pltpu.VMEM((8 * rows, hid), BF),
            pltpu.VMEM((rows, dim), F32),
            pltpu.VMEM(last, BF),
            pltpu.VMEM(last, BF),
            pltpu.VMEM(last[2:], BF),
            pltpu.VMEM(last, BF),
            dma((64,)), dma((200,)), dma((NZ, 2, 2)), dma((NZ, NY - 1)), dma((NZ + 1, 2)),
            dma((NZ,)), dma((NZ, NY - 1)), dma((NZ, 2)), dma((2, NZ - 1, 2)), dma((NY, 2)), dma((NY, 2)),
        ],
        compiler_params=pltpu.CompilerParams(
            collective_id=0, has_side_effects=True, vmem_limit_bytes=62 * 1024 * 1024
        ),
    )(tokens, ids, probs, wg, wu, wd, sg, su, sd)


def body(tokens, expert_ids, gate_probs, w_gate, w_up, w_down, shared_gate, shared_up, shared_down):
    dim = tokens.shape[1]
    stacked = lambda w: jnp.swapaxes(w, 1, 2).reshape(-1, dim)
    return layer(
        tokens, expert_ids.T, gate_probs.T, stacked(w_gate), stacked(w_up), w_down.reshape(-1, dim),
        shared_gate.T, shared_up.T, shared_down,
    )


def solution(mesh):
    torus = Mesh(mesh.devices.reshape(NZ, 2, 2, 4, 2), ("z", "xl", "c", "y", "xh"))
    e, t = ("z", "xl", "c"), ("y", "xh")
    return jax.shard_map(
        body,
        mesh=torus,
        in_specs=(
            P(e, None), P(), P(),
            P(e, None, t), P(e, None, t), P(e, t, None),
            P(None, t), P(None, t), P(t, None),
        ),
        out_specs=P(e, None),
        check_vma=False,
    )
```

```python
import jax
import jax.numpy as jnp
from jax import lax
from jax.experimental import pallas as pl
from jax.experimental.pallas import tpu as pltpu
from jax.sharding import Mesh
from jax.sharding import PartitionSpec as P

MESH = pl.DeviceIdType.MESH
NZ, NY = 8, 4
OFFSETS = (0, -1, 1, -2, 2, -3, 3, 4)
SLOT = {d % NZ: s for s, d in enumerate(OFFSETS)}
BF, F32 = jnp.bfloat16, jnp.float32
GA, GR = 512, 512
NT_DIMS = (((1,), (1,)), ((), ()))


def kernel(
    tokens, ids, probs, wg, wu, wd, sg, su, sd, out,
    gath, part, yy, xx, zin, zout, wguv, wdv, sguv, sdv, idv, prv, wsc, hbuf, sbuf,
    tsb, tsi, fin, agi,
    loc_sem, snd_sem, wt_sem, ag_sem, ya_sem, yr_sem, xx_sem, zin_sem, ts_sem, ta_sem,
):
    z, xl, c = lax.axis_index("z"), lax.axis_index("xl"), lax.axis_index("c")
    y, xh = lax.axis_index("y"), lax.axis_index("xh")
    rows, dim = tokens.shape
    half, quarter = rows // 2, rows // 4
    hid = wg.shape[0]
    width = hid // 2
    sa, sr = GA // NY, GR // NY
    ca, cr = dim - GA, dim - GR
    aw, rw = ca + sa, cr + sr
    zup, zdn = {"z": lax.rem(z + 1, NZ)}, {"z": lax.rem(z + NZ - 1, NZ)}
    xup = {"xl": 1 - xl, "xh": lax.rem(xh + xl, 2)}
    xdn = {"xl": 1 - xl, "xh": lax.rem(xh + 1 - xl, 2)}
    mate = {"c": 1 - c}
    yat = [lax.rem(y + i, NY) for i in range(NY)]
    peers = [(yat[i], lax.rem(xh + j, 2), i, j) for i in range(NY) for j in (0, 1)][1:]
    other = 1 - xl

    local = []

    def load(src, dst):
        cp = pltpu.make_async_copy(src, dst, loc_sem.at[len(local)])
        cp.start()
        local.append(cp)
        return cp

    def load_turned(src, dst, common, size):
        cps = [load(src.at[:, pl.ds(0, common)], dst.at[:, pl.ds(0, common)])]
        for i in range(NY if size else 0):
            at = pl.multiple_of(common + yat[i] * size, 128)
            cps.append(load(src.at[:, pl.ds(at, size)], dst.at[:, pl.ds(common + i * size, size)]))
        return cps

    def at_rows(ref, first):
        return ref.at[pl.ds(first, hid)]

    tok_cp = load_turned(tokens, gath.at[0, xl], ca, sa)
    rt_cp = (
        load_turned(wg, at_rows(wguv, 0), ca, sa)
        + load_turned(wu, at_rows(wguv, 2 * hid), ca, sa)
        + load_turned(wd, at_rows(wdv, 0), cr, sr)
    )
    id_cp = [load(ids, idv), load(probs, prv)]
    sh_cp = (
        load_turned(sg, at_rows(sguv, 0), ca, sa)
        + load_turned(su, at_rows(sguv, hid), ca, sa)
        + load_turned(sd, sdv, cr, sr)
    )

    barrier = pltpu.get_barrier_semaphore()
    greeted = [zup, zdn, xup, xdn, mate] + [{"y": yp, "xh": xp} for yp, xp, _, _ in peers]
    for dev in greeted:
        pl.semaphore_signal(barrier, inc=1, device_id=dev, device_id_type=MESH)
    with jax.named_scope("barrier"):
        pl.semaphore_wait(barrier, len(greeted))

    sent = []

    def send(src, dst, sem, dev):
        cp = pltpu.make_async_remote_copy(
            src_ref=src, dst_ref=dst, send_sem=snd_sem.at[len(sent)], recv_sem=sem,
            device_id=dev, device_id_type=MESH,
        )
        cp.start()
        sent.append(cp)

    def arrive(dst, sem):
        pltpu.make_async_remote_copy(
            src_ref=dst, dst_ref=dst, send_sem=snd_sem.at[0], recv_sem=sem,
            device_id=mate, device_id_type=MESH,
        ).wait_recv()

    def slots(k):
        return (0,) if k == 0 else (7,) if k == 4 else (2 * k - 1, 2 * k)

    def unit(slot, b, h):
        return gath.at[slot, b, pl.ds(h * half, half), pl.ds(0, aw)]

    def hop(offset, h, up):
        nxt = SLOT[(offset - 1 if up else offset + 1) % NZ]
        send(unit(SLOT[offset % NZ], xl, h), unit(nxt, xl, h), ag_sem.at[nxt, 0, h], zup if up else zdn)

    def across(slot, h):
        send(unit(slot, xl, h), unit(slot, xl, h), ag_sem.at[slot, 1, h], xup if h == 0 else xdn)

    def gather_z(k):
        for h in (0, 1):
            for up in (True, False):
                if k == 4 and up != (h == 0):
                    continue
                offset = -k if up else k
                slot = SLOT[offset % NZ]
                arrive(unit(slot, xl, h), ag_sem.at[slot, 0, h])
                if k < 3 or (k == 3 and up == (h == 0)):
                    hop(offset, h, up)
                across(slot, h)

    def piece(slot, i):
        blocks = pl.ds(other, 1) if slot == 0 else pl.ds(0, 2)
        return gath.at[slot, blocks, :, pl.ds(ca + i * sa, sa)]

    def gather_x(k):
        for slot in slots(k):
            for h in (0, 1):
                arrive(unit(slot, other, h), ag_sem.at[slot, 1, h])
            for i in range(1, NY if GA else 1):
                send(piece(slot, 0), piece(slot, NY - i), ya_sem.at[slot, NY - i - 1], {"y": yat[i]})

    def gather_y(k):
        for slot in slots(k) if GA else ():
            for i in range(1, NY):
                arrive(piece(slot, i), ya_sem.at[slot, i - 1])

    def ffn(x, gu_ref, d_ref, scales, write):
        m = x.shape[0]
        n = d_ref.shape[0]
        gu = lax.dot_general(gu_ref[...], x, NT_DIMS, preferred_element_type=F32)
        if scales is None:
            g, u = gu[:n], gu[n:]
            h = g / (1.0 + jnp.exp(-g)) * u
        else:
            hs = []
            for j, scale in enumerate(scales):
                g, u = gu[j * width : (j + 1) * width], gu[n + j * width : n + (j + 1) * width]
                hs.append(g / (1.0 + jnp.exp(-g)) * u * scale)
            h = jnp.concatenate(hs, axis=0)
        hbuf[pl.ds(0, m), pl.ds(0, n)] = h.T.astype(BF)

        @pl.loop(0, 4)
        def _(i):
            cols = pl.ds(pl.multiple_of(i * 512, 512), 512)
            write(cols, jnp.dot(hbuf[pl.ds(0, m), pl.ds(0, n)], d_ref[:, cols], preferred_element_type=F32))

    def weigh():
        group, pair = 4 * rows, 2 * rows
        lane = lax.broadcasted_iota(jnp.int32, (8, pair), 1)
        for slot, offset in enumerate(OFFSETS):
            gz = lax.rem(z + offset + NZ, NZ)
            lanes = pl.ds(pl.multiple_of(gz * group, group), group)
            for j in range(4):
                expert = (z * 4 + xl * 2 + (c if j < 2 else 1 - c)) * 2 + j % 2
                row = jnp.sum(jnp.where(idv[:, lanes] == expert, prv[:, lanes], 0.0), axis=0, keepdims=True)
                lo, hi = (jnp.broadcast_to(row[:, at : at + pair], (8, pair)) for at in (0, pair))
                even = jnp.where(lane < rows, lo, pltpu.roll(hi, rows, 1))
                odd = jnp.where(lane < rows, pltpu.roll(lo, rows, 1), hi)
                wsc[j : j + 1, slot * pair : (slot + 1) * pair] = jnp.where(c == 0, even, odd)[0:1]

    def compute(k):
        ss = slots(k)
        s0, ns = ss[0], len(ss)
        pair = 2 * rows
        scales = [wsc[j : j + 1, s0 * pair : (s0 + ns) * pair] for j in range(4)]

        def write(cols, p):
            part[pl.ds(s0, ns), :, :, cols] = p.astype(BF).reshape(ns, 2, rows, 512)

        ffn(gath[pl.ds(s0, ns)].reshape(ns * pair, dim), wguv, wdv, scales, write)
        if k == 0:
            part[0, xl] = (part[0, xl].astype(F32) + sbuf[...]).astype(BF)

    sides = ((0, xup), (1, xdn))

    def x_send(slot, h, dev, lo, n, which):
        r = pl.ds(h * half, half)
        cols = pl.ds(lo, n)
        send(part.at[slot, other, r, cols], xx.at[slot, r, cols], xx_sem.at[slot, h, which], dev)

    def swap_y(k):
        for slot in slots(k):
            for h, dev in sides:
                x_send(slot, h, dev, 0, cr, 0)
            for i in range(1, NY if GR else 1):
                send(
                    part.at[slot, :, :, pl.ds(cr + i * sr, sr)], yy.at[slot, NY - i - 1],
                    yr_sem.at[slot, NY - i - 1], {"y": yat[i]},
                )

    def sliced(slot, b, r):
        v = part[slot, b, r, cr:rw].astype(F32)
        for i in range(NY - 1):
            v = v + yy[slot, i, b, r].astype(F32)
        return v

    def summed(slot, r):
        common = part[slot, xl, r, 0:cr].astype(F32)
        return [common, sliced(slot, xl, r)] if GR else [common]

    bounds = [(0, cr), (cr, rw)][: 2 if GR else 1]

    def swap_x(k):
        for slot in slots(k) if GR else ():
            for i in range(NY - 1):
                arrive(yy.at[slot, i], yr_sem.at[slot, i])
            part[slot, other, :, cr:rw] = sliced(slot, other, slice(None)).astype(BF)
            for h, dev in sides:
                x_send(slot, h, dev, cr, sr, 1)

    def x_arrive(slot, h):
        r = pl.ds(h * half, half)
        for which, (lo, hi) in enumerate(bounds):
            arrive(xx.at[slot, r, pl.ds(lo, hi - lo)], xx_sem.at[slot, h, which])

    def ring(s):
        for h, up in ((0, True), (1, False)):
            x_arrive(SLOT[(-s if up else s) % NZ], h)
        for q in (0, 1):
            r = pl.ds(q * quarter, quarter)
            for h, up in ((0, True), (1, False)):
                slot = SLOT[(-s if up else s) % NZ]
                full = pl.ds(h * half + q * quarter, quarter)
                if s > 1:
                    arrive(zin.at[h, s - 2, r], zin_sem.at[h, s - 2, q])
                for (lo, hi), v in zip(bounds, summed(slot, full)):
                    v = v + xx[slot, full, lo:hi].astype(F32)
                    if s > 1:
                        v = v + zin[h, s - 2, r, lo:hi].astype(F32)
                    zout[h, s - 1, r, lo:hi] = v.astype(BF)
                send(zout.at[h, s - 1, r], zin.at[h, s - 1, r], zin_sem.at[h, s - 1, q], zup if up else zdn)

    for cp in tok_cp:
        cp.wait()
    for h in (0, 1):
        hop(0, h, True)
        hop(0, h, False)
        across(0, h)
    for cp in rt_cp:
        cp.wait()
    moved = ((wguv, 0), (wguv, 2 * hid), (wdv, 0))
    for i, (ref, at) in enumerate(moved):
        send(at_rows(ref, at), at_rows(ref, at + hid), wt_sem.at[i], mate)
    for cp in id_cp + sh_cp:
        cp.wait()

    def write_shared(cols, p):
        sbuf[:, cols] = p

    with jax.named_scope("shared"):
        ffn(gath[0, xl], sguv, sdv, None, write_shared)
    with jax.named_scope("weigh"):
        weigh()

    def weights():
        for i, (ref, at) in enumerate(moved):
            arrive(at_rows(ref, at + hid), wt_sem.at[i])

    with jax.named_scope("s00_gz1"):
        gather_z(1)
    with jax.named_scope("s01_gx0"):
        gather_x(0)
    with jax.named_scope("s02_gy0"):
        gather_y(0)
    with jax.named_scope("s03_w"):
        weights()
    with jax.named_scope("s04_c0"):
        compute(0)
    with jax.named_scope("s05_gz2"):
        gather_z(2)
    with jax.named_scope("s06_gx1"):
        gather_x(1)
    with jax.named_scope("s07_gy1"):
        gather_y(1)
    with jax.named_scope("s08_c1"):
        compute(1)
    with jax.named_scope("s09_sy1"):
        swap_y(1)
    with jax.named_scope("s10_gz3"):
        gather_z(3)
    with jax.named_scope("s11_gx2"):
        gather_x(2)
    with jax.named_scope("s12_sx1"):
        swap_x(1)
    with jax.named_scope("s13_gy2"):
        gather_y(2)
    with jax.named_scope("s14_c2"):
        compute(2)
    with jax.named_scope("s15_sy2"):
        swap_y(2)
    with jax.named_scope("s16_gz4"):
        gather_z(4)
    with jax.named_scope("s17_gx3"):
        gather_x(3)
    with jax.named_scope("s18_r1"):
        ring(1)
    with jax.named_scope("s19_sx2"):
        swap_x(2)
    with jax.named_scope("s20_gy3"):
        gather_y(3)
    with jax.named_scope("s21_c3"):
        compute(3)
    with jax.named_scope("s22_sy3"):
        swap_y(3)
    with jax.named_scope("s23_gx4"):
        gather_x(4)
    with jax.named_scope("s24_r2"):
        ring(2)
    with jax.named_scope("s25_sx3"):
        swap_x(3)
    with jax.named_scope("s26_gy4"):
        gather_y(4)
    with jax.named_scope("s27_c4"):
        compute(4)
    with jax.named_scope("s28_sy4"):
        swap_y(4)
    with jax.named_scope("s29_sy0"):
        swap_y(0)
    with jax.named_scope("s30_r3"):
        ring(3)
    with jax.named_scope("s31_sx4"):
        swap_x(4)
    with jax.named_scope("s32_sx0"):
        swap_x(0)
    with jax.named_scope("s33_r4"):
        ring(4)
    with jax.named_scope("s34_r5"):
        ring(5)
    with jax.named_scope("s35_r6"):
        ring(6)
    with jax.named_scope("s36_r7"):
        ring(7)
    cw = cr // NY
    with jax.named_scope("final"):
        for h in (0, 1):
            r = pl.ds(h * half, half)
            x_arrive(0, h)
            for q in (0, 1):
                rq = pl.ds(q * quarter, quarter)
                arrive(zin.at[h, NZ - 2, rq], zin_sem.at[h, NZ - 2, q])
            for (lo, hi), v in zip(bounds, summed(0, r)):
                v = (v + xx[0, r, lo:hi].astype(F32) + zin[h, NZ - 2, :, lo:hi].astype(F32)).astype(BF)
                if lo == 0:
                    for i in range(NY):
                        tsb[i, h, :, 0:cw] = v[:, i * cw : (i + 1) * cw]
                else:
                    tsb[y, h, :, cw : cw + sr] = v
    with jax.named_scope("tensor_sum"):
        for yp, xp, i, j in peers:
            n = cw + sr if i == 0 else cw
            send(
                tsb.at[yp, xp, :, pl.ds(0, n)], tsi.at[(NY - i) % NY, j, :, pl.ds(0, n)],
                ts_sem.at[(NY - i) % NY, j], {"y": yp, "xh": xp},
            )
        acc = tsb[y, xh, :, 0:cw].astype(F32)
        for _, _, i, j in peers:
            n = cw + sr if i == 0 else cw
            arrive(tsi.at[i, j, :, pl.ds(0, n)], ts_sem.at[i, j])
            acc = acc + tsi[i, j, :, 0:cw].astype(F32)
        fin[:, 0:cw] = acc.astype(BF)
        if GR:
            fin[:, cw : cw + sr] = (
                tsb[y, xh, :, cw : cw + sr].astype(F32) + tsi[0, 1, :, cw : cw + sr].astype(F32)
            ).astype(BF)
    with jax.named_scope("tensor_all"):
        for yp, xp, i, j in peers:
            send(fin, agi.at[y, xh], ta_sem.at[(NY - i) % NY, j], {"y": yp, "xh": xp})
        agi[y, xh] = fin[...]
        for yp, xp, i, j in peers:
            arrive(agi.at[yp, xp], ta_sem.at[i, j])
        for i in range(NY):
            for j in (0, 1):
                r = pl.ds(j * half, half)
                out[r, i * cw : (i + 1) * cw] = agi[i, j, :, 0:cw]
                if GR:
                    out[r, cr + i * sr : cr + (i + 1) * sr] = agi[i, j, :, cw : cw + sr]
    with jax.named_scope("sends"):
        for cp in sent:
            cp.wait_send()


def layer(tokens, ids, probs, wg, wu, wd, sg, su, sd):
    rows, dim = tokens.shape
    hid = sg.shape[0]
    rw = dim - GR + GR // NY
    any_spec = pl.BlockSpec(memory_space=pl.ANY)
    dma = pltpu.SemaphoreType.DMA
    last = (NY, 2, rows // 2, dim // NY)
    return pl.pallas_call(
        kernel,
        out_shape=jax.ShapeDtypeStruct((rows, dim), BF),
        in_specs=[any_spec] * 9,
        out_specs=pl.BlockSpec(memory_space=pltpu.VMEM),
        scratch_shapes=[
            pltpu.VMEM((NZ, 2, rows, dim), BF),
            pltpu.VMEM((NZ, 2, rows, dim), BF),
            pltpu.VMEM((NZ, NY - 1, 2, rows, max(GR // NY, 128)), BF),
            pltpu.VMEM((NZ, rows, rw), BF),
            pltpu.VMEM((2, NZ - 1, rows // 2, rw), BF),
            pltpu.VMEM((2, NZ - 1, rows // 2, rw), BF),
            pltpu.VMEM((4 * hid, dim), BF),
            pltpu.VMEM((2 * hid, dim), BF),
            pltpu.VMEM((2 * hid, dim), BF),
            pltpu.VMEM((hid, dim), BF),
            pltpu.VMEM(ids.shape, jnp.int32),
            pltpu.VMEM(probs.shape, F32),
            pltpu.VMEM((8, NZ * 2 * rows), F32),
            pltpu.VMEM((4 * rows, 2 * hid), BF),
            pltpu.VMEM((rows, dim), F32),
            pltpu.VMEM(last, BF),
            pltpu.VMEM(last, BF),
            pltpu.VMEM(last[2:], BF),
            pltpu.VMEM(last, BF),
            dma((64,)), dma((200,)), dma((3,)), dma((NZ, 2, 2)), dma((NZ, NY - 1)),
            dma((NZ, NY - 1)), dma((NZ, 2, 2)), dma((2, NZ - 1, 2)), dma((NY, 2)), dma((NY, 2)),
        ],
        compiler_params=pltpu.CompilerParams(
            collective_id=0, has_side_effects=True, vmem_limit_bytes=62 * 1024 * 1024
        ),
    )(tokens, ids, probs, wg, wu, wd, sg, su, sd)


def body(tokens, expert_ids, gate_probs, w_gate, w_up, w_down, shared_gate, shared_up, shared_down):
    dim = tokens.shape[1]
    stacked = lambda w: jnp.swapaxes(w, 1, 2).reshape(-1, dim)
    return layer(
        tokens, expert_ids.T, gate_probs.T, stacked(w_gate), stacked(w_up), w_down.reshape(-1, dim),
        shared_gate.T, shared_up.T, shared_down,
    )


def solution(mesh):
    torus = Mesh(mesh.devices.reshape(NZ, 2, 2, 4, 2), ("z", "xl", "c", "y", "xh"))
    e, t = ("z", "xl", "c"), ("y", "xh")
    return jax.shard_map(
        body,
        mesh=torus,
        in_specs=(
            P(e, None), P(), P(),
            P(e, None, t), P(e, None, t), P(e, t, None),
            P(None, t), P(None, t), P(t, None),
        ),
        out_specs=P(e, None),
        check_vma=False,
    )
```

```python
import jax
import jax.numpy as jnp
from jax import lax
from jax.experimental import pallas as pl
from jax.experimental.pallas import tpu as pltpu
from jax.sharding import Mesh
from jax.sharding import PartitionSpec as P

MESH = pl.DeviceIdType.MESH
NZ, NY = 8, 4
OFFSETS = (0, -1, 1, -2, 2, -3, 3, 4)
SLOT = {d % NZ: s for s, d in enumerate(OFFSETS)}
BF, F32 = jnp.bfloat16, jnp.float32
GA, GR = 512, 512
NT_DIMS = (((1,), (1,)), ((), ()))


def kernel(
    tokens, ids, probs, wg, wu, wd, sg, su, sd, out,
    gath, part, yy, xx, zin, zout, wguv, wdv, sguv, sdv, idv, prv, wsc, hbuf, sbuf,
    tsb, tsi, fin, agi,
    loc_sem, snd_sem, wt_sem, ag_sem, ax_sem, ya_sem, yr_sem, xx_sem, zin_sem, ts_sem, ta_sem,
):
    z, xl, c = lax.axis_index("z"), lax.axis_index("xl"), lax.axis_index("c")
    y, xh = lax.axis_index("y"), lax.axis_index("xh")
    rows, dim = tokens.shape
    half, quarter = rows // 2, rows // 4
    hid = wg.shape[0]
    width = hid // 2
    sa, sr = GA // NY, GR // NY
    ca, cr = dim - GA, dim - GR
    aw, rw = ca + sa, cr + sr
    zup, zdn = {"z": lax.rem(z + 1, NZ)}, {"z": lax.rem(z + NZ - 1, NZ)}
    xup = {"xl": 1 - xl, "xh": lax.rem(xh + xl, 2)}
    xdn = {"xl": 1 - xl, "xh": lax.rem(xh + 1 - xl, 2)}
    mate = {"c": 1 - c}
    yat = [lax.rem(y + i, NY) for i in range(NY)]
    peers = [(yat[i], lax.rem(xh + j, 2), i, j) for i in range(NY) for j in (0, 1)][1:]
    other = 1 - xl

    local = []

    def load(src, dst, common=None, size=0):
        sem = loc_sem.at[len(local)]
        if size:
            pltpu.make_async_copy(src.at[:, pl.ds(0, common)], dst.at[:, pl.ds(0, common)], sem).start()
            for i in range(NY):
                at = pl.multiple_of(common + yat[i] * size, 128)
                pltpu.make_async_copy(
                    src.at[:, pl.ds(at, size)], dst.at[:, pl.ds(common + i * size, size)], sem
                ).start()
        else:
            pltpu.make_async_copy(src, dst, sem).start()
        local.append(pltpu.make_async_copy(src, dst, sem))
        return local[-1:]

    def at_rows(ref, first):
        return ref.at[pl.ds(first, hid)]

    tok_cp = load(tokens, gath.at[0, xl], ca, sa)
    rt_cp = (
        load(wg, at_rows(wguv, 0), ca, sa)
        + load(wu, at_rows(wguv, 2 * hid), ca, sa)
        + load(wd, at_rows(wdv, 0), cr, sr)
    )
    id_cp = load(ids, idv) + load(probs, prv)
    sh_cp = (
        load(sg, at_rows(sguv, 0), ca, sa)
        + load(su, at_rows(sguv, hid), ca, sa)
        + load(sd, sdv, cr, sr)
    )

    barrier = pltpu.get_barrier_semaphore()
    greeted = [zup, zdn, xup, xdn, mate] + [{"y": yp, "xh": xp} for yp, xp, _, _ in peers]
    for dev in greeted:
        pl.semaphore_signal(barrier, inc=1, device_id=dev, device_id_type=MESH)
    with jax.named_scope("barrier"):
        pl.semaphore_wait(barrier, len(greeted))

    kinds = {}

    def send(kind, src, dst, sem, dev):
        pltpu.make_async_remote_copy(
            src_ref=src, dst_ref=dst, send_sem=snd_sem.at[kinds.setdefault(kind, len(kinds))],
            recv_sem=sem, device_id=dev, device_id_type=MESH,
        ).start()

    def all_sent(kind, whole):
        pltpu.make_async_remote_copy(
            src_ref=whole, dst_ref=whole, send_sem=snd_sem.at[kinds[kind]], recv_sem=snd_sem.at[0],
            device_id=mate, device_id_type=MESH,
        ).wait_send()

    def arrive(dst, sem):
        pltpu.make_async_remote_copy(
            src_ref=dst, dst_ref=dst, send_sem=snd_sem.at[0], recv_sem=sem,
            device_id=mate, device_id_type=MESH,
        ).wait_recv()

    def slots(k):
        return (0,) if k == 0 else (7,) if k == 4 else (2 * k - 1, 2 * k)

    def unit(slot, b, h):
        return gath.at[slot, b, pl.ds(h * half, half), pl.ds(0, aw)]

    def hop(offset, h, up):
        nxt = SLOT[(offset - 1 if up else offset + 1) % NZ]
        send("z", unit(SLOT[offset % NZ], xl, h), unit(nxt, xl, h), ag_sem.at[nxt, h], zup if up else zdn)

    def across(slot, h):
        send("x", unit(slot, xl, h), unit(slot, xl, h), ax_sem.at[slot], xup if h == 0 else xdn)

    def gather_z(k):
        for h in (0, 1):
            for up in (True, False):
                if k == 4 and up != (h == 0):
                    continue
                offset = -k if up else k
                slot = SLOT[offset % NZ]
                arrive(unit(slot, xl, h), ag_sem.at[slot, h])
                if k < 3 or (k == 3 and up == (h == 0)):
                    hop(offset, h, up)
                across(slot, h)

    def piece(slot, i, n=1):
        blocks = pl.ds(other, 1) if slot == 0 else pl.ds(0, 2)
        return gath.at[slot, blocks, :, pl.ds(ca + i * sa, n * sa)]

    def gather_x(k):
        for slot in slots(k):
            arrive(gath.at[slot, other, :, pl.ds(0, aw)], ax_sem.at[slot])
            for i in range(1, NY if GA else 1):
                send("y" if slot else "y0", piece(slot, 0), piece(slot, NY - i), ya_sem.at[slot], {"y": yat[i]})

    def gather_y(k):
        for slot in slots(k) if GA else ():
            arrive(piece(slot, 1, NY - 1), ya_sem.at[slot])

    def ffn(x, gu_ref, d_ref, scales, write):
        m = x.shape[0]
        n = d_ref.shape[0]
        gu = lax.dot_general(gu_ref[...], x, NT_DIMS, preferred_element_type=F32)
        if scales is None:
            g, u = gu[:n], gu[n:]
            h = g / (1.0 + jnp.exp(-g)) * u
        else:
            hs = []
            for j, scale in enumerate(scales):
                g, u = gu[j * width : (j + 1) * width], gu[n + j * width : n + (j + 1) * width]
                hs.append(g / (1.0 + jnp.exp(-g)) * u * scale)
            h = jnp.concatenate(hs, axis=0)
        hbuf[pl.ds(0, m), pl.ds(0, n)] = h.T.astype(BF)

        @pl.loop(0, 4)
        def _(i):
            cols = pl.ds(pl.multiple_of(i * 512, 512), 512)
            write(cols, jnp.dot(hbuf[pl.ds(0, m), pl.ds(0, n)], d_ref[:, cols], preferred_element_type=F32))

    def weigh():
        group, pair = 4 * rows, 2 * rows
        lane = lax.broadcasted_iota(jnp.int32, (8, pair), 1)
        for slot, offset in enumerate(OFFSETS):
            gz = lax.rem(z + offset + NZ, NZ)
            lanes = pl.ds(pl.multiple_of(gz * group, group), group)
            for j in range(4):
                expert = (z * 4 + xl * 2 + (c if j < 2 else 1 - c)) * 2 + j % 2
                row = jnp.sum(jnp.where(idv[:, lanes] == expert, prv[:, lanes], 0.0), axis=0, keepdims=True)
                lo, hi = (jnp.broadcast_to(row[:, at : at + pair], (8, pair)) for at in (0, pair))
                even = jnp.where(lane < rows, lo, pltpu.roll(hi, rows, 1))
                odd = jnp.where(lane < rows, pltpu.roll(lo, rows, 1), hi)
                wsc[j : j + 1, slot * pair : (slot + 1) * pair] = jnp.where(c == 0, even, odd)[0:1]

    def compute(k):
        ss = slots(k)
        s0, ns = ss[0], len(ss)
        pair = 2 * rows
        scales = [wsc[j : j + 1, s0 * pair : (s0 + ns) * pair] for j in range(4)]

        def write(cols, p):
            part[pl.ds(s0, ns), :, :, cols] = p.astype(BF).reshape(ns, 2, rows, 512)

        ffn(gath[pl.ds(s0, ns)].reshape(ns * pair, dim), wguv, wdv, scales, write)
        if k == 0:
            part[0, xl] = (part[0, xl].astype(F32) + sbuf[...]).astype(BF)

    sides = ((0, xup), (1, xdn))

    def x_send(slot, h, dev, lo, n, which):
        r = pl.ds(h * half, half)
        cols = pl.ds(lo, n)
        send(f"xx{which}", part.at[slot, other, r, cols], xx.at[slot, r, cols], xx_sem.at[slot, h], dev)

    def swap_y(k):
        for slot in slots(k):
            for h, dev in sides:
                x_send(slot, h, dev, 0, cr, 0)
            for i in range(1, NY if GR else 1):
                send(
                    "yy", part.at[slot, :, :, pl.ds(cr + i * sr, sr)], yy.at[slot, NY - i - 1],
                    yr_sem.at[slot], {"y": yat[i]},
                )

    def sliced(slot, b, r):
        v = part[slot, b, r, cr:rw].astype(F32)
        for i in range(NY - 1):
            v = v + yy[slot, i, b, r].astype(F32)
        return v

    def summed(slot, r):
        common = part[slot, xl, r, 0:cr].astype(F32)
        return [common, sliced(slot, xl, r)] if GR else [common]

    bounds = [(0, cr), (cr, rw)][: 2 if GR else 1]

    def swap_x(k):
        for slot in slots(k) if GR else ():
            arrive(yy.at[slot], yr_sem.at[slot])
            part[slot, other, :, cr:rw] = sliced(slot, other, slice(None)).astype(BF)
            for h, dev in sides:
                x_send(slot, h, dev, cr, sr, 1)

    def x_arrive(slot, h):
        r = pl.ds(h * half, half)
        arrive(xx.at[slot, r], xx_sem.at[slot, h])

    def ring(s):
        for h, up in ((0, True), (1, False)):
            x_arrive(SLOT[(-s if up else s) % NZ], h)
        for q in (0, 1):
            r = pl.ds(q * quarter, quarter)
            for h, up in ((0, True), (1, False)):
                slot = SLOT[(-s if up else s) % NZ]
                full = pl.ds(h * half + q * quarter, quarter)
                if s > 1:
                    arrive(zin.at[h, s - 2, r], zin_sem.at[h, s - 2, q])
                for (lo, hi), v in zip(bounds, summed(slot, full)):
                    v = v + xx[slot, full, lo:hi].astype(F32)
                    if s > 1:
                        v = v + zin[h, s - 2, r, lo:hi].astype(F32)
                    zout[h, s - 1, r, lo:hi] = v.astype(BF)
                send("zz", zout.at[h, s - 1, r], zin.at[h, s - 1, r], zin_sem.at[h, s - 1, q], zup if up else zdn)

    for cp in tok_cp:
        cp.wait()
    for h in (0, 1):
        hop(0, h, True)
        hop(0, h, False)
        across(0, h)
    for cp in rt_cp:
        cp.wait()
    moved = ((wguv, 0), (wguv, 2 * hid), (wdv, 0))
    for i, (ref, at) in enumerate(moved):
        send(f"w{i}", at_rows(ref, at), at_rows(ref, at + hid), wt_sem.at[i], mate)
    for cp in id_cp + sh_cp:
        cp.wait()

    def write_shared(cols, p):
        sbuf[:, cols] = p

    with jax.named_scope("shared"):
        ffn(gath[0, xl], sguv, sdv, None, write_shared)
    with jax.named_scope("weigh"):
        weigh()

    def weights():
        for i, (ref, at) in enumerate(moved):
            arrive(at_rows(ref, at + hid), wt_sem.at[i])

    with jax.named_scope("s00_gz1"):
        gather_z(1)
    with jax.named_scope("s01_gx0"):
        gather_x(0)
    with jax.named_scope("s02_gz2"):
        gather_z(2)
    with jax.named_scope("s03_gx1"):
        gather_x(1)
    with jax.named_scope("s04_gy0"):
        gather_y(0)
    with jax.named_scope("s05_w"):
        weights()
    with jax.named_scope("s06_c0"):
        compute(0)
    with jax.named_scope("s07_gz3"):
        gather_z(3)
    with jax.named_scope("s08_gx2"):
        gather_x(2)
    with jax.named_scope("s09_gy1"):
        gather_y(1)
    with jax.named_scope("s10_c1"):
        compute(1)
    with jax.named_scope("s11_sy1"):
        swap_y(1)
    with jax.named_scope("s12_gz4"):
        gather_z(4)
    with jax.named_scope("s13_gx3"):
        gather_x(3)
    with jax.named_scope("s14_gy2"):
        gather_y(2)
    with jax.named_scope("s15_c2"):
        compute(2)
    with jax.named_scope("s16_sy2"):
        swap_y(2)
    with jax.named_scope("s17_sx1"):
        swap_x(1)
    with jax.named_scope("s18_gx4"):
        gather_x(4)
    with jax.named_scope("s19_gy3"):
        gather_y(3)
    with jax.named_scope("s20_c3"):
        compute(3)
    with jax.named_scope("s21_sy3"):
        swap_y(3)
    with jax.named_scope("s22_r1"):
        ring(1)
    with jax.named_scope("s23_sx2"):
        swap_x(2)
    with jax.named_scope("s24_gy4"):
        gather_y(4)
    with jax.named_scope("s25_c4"):
        compute(4)
    with jax.named_scope("s26_sy4"):
        swap_y(4)
    with jax.named_scope("s27_sy0"):
        swap_y(0)
    with jax.named_scope("s28_sx3"):
        swap_x(3)
    with jax.named_scope("s29_r2"):
        ring(2)
    with jax.named_scope("s30_sx4"):
        swap_x(4)
    with jax.named_scope("s31_sx0"):
        swap_x(0)
    with jax.named_scope("s32_r3"):
        ring(3)
    with jax.named_scope("s33_r4"):
        ring(4)
    with jax.named_scope("s34_r5"):
        ring(5)
    with jax.named_scope("s35_r6"):
        ring(6)
    with jax.named_scope("s36_r7"):
        ring(7)
    cw = cr // NY
    with jax.named_scope("final"):
        for h in (0, 1):
            r = pl.ds(h * half, half)
            x_arrive(0, h)
            for q in (0, 1):
                rq = pl.ds(q * quarter, quarter)
                arrive(zin.at[h, NZ - 2, rq], zin_sem.at[h, NZ - 2, q])
            for (lo, hi), v in zip(bounds, summed(0, r)):
                v = (v + xx[0, r, lo:hi].astype(F32) + zin[h, NZ - 2, :, lo:hi].astype(F32)).astype(BF)
                if lo == 0:
                    for i in range(NY):
                        tsb[2 * i + h, :, 0:cw] = v[:, i * cw : (i + 1) * cw]
                else:
                    tsb[2 * y + h, :, cw : cw + sr] = v
    me = 2 * y + xh
    with jax.named_scope("tensor_sum"):
        for yp, xp, i, j in peers:
            n = cw + sr if i == 0 else cw
            send(
                "t0" if i == 0 else "t1", tsb.at[2 * yp + xp, :, pl.ds(0, n)],
                tsi.at[2 * ((NY - i) % NY) + j, :, pl.ds(0, n)],
                ts_sem.at[min(i, 1)], {"y": yp, "xh": xp},
            )
        mate_sum, far_sums = tsi.at[1, :, pl.ds(0, cw + sr)], tsi.at[pl.ds(2, 6), :, pl.ds(0, cw)]
        arrive(mate_sum, ts_sem.at[0])
        acc = tsb[me, :, 0:cw].astype(F32) + tsi[1, :, 0:cw].astype(F32)
        if GR:
            fin[:, cw : cw + sr] = (
                tsb[me, :, cw : cw + sr].astype(F32) + tsi[1, :, cw : cw + sr].astype(F32)
            ).astype(BF)
        arrive(far_sums, ts_sem.at[1])
        for i in range(2, 8):
            acc = acc + tsi[i, :, 0:cw].astype(F32)
        fin[:, 0:cw] = acc.astype(BF)
    with jax.named_scope("tensor_all"):
        for yp, xp, i, j in peers:
            send("t2", fin, agi.at[me], ta_sem.at[0], {"y": yp, "xh": xp})
        agi[me] = fin[...]
        others = agi.at[pl.ds(0, 7)]
        arrive(others, ta_sem.at[0])
        for i in range(NY):
            for j in (0, 1):
                r = pl.ds(j * half, half)
                out[r, i * cw : (i + 1) * cw] = agi[2 * i + j, :, 0:cw]
                if GR:
                    out[r, cr + i * sr : cr + (i + 1) * sr] = agi[2 * i + j, :, cw : cw + sr]
    all_sent("z", gath.at[pl.ds(0, 7), 0, :, pl.ds(0, aw)])
    all_sent("x", gath.at[:, 0, :, pl.ds(0, aw)])
    if GA:
        all_sent("y", gath.at[pl.ds(0, 7), :, :, pl.ds(0, 3 * sa)])
        all_sent("y0", gath.at[0, 0, :, pl.ds(0, 3 * sa)])
    all_sent("xx0", part.at[:, 0, :, pl.ds(0, cr)])
    if GR:
        all_sent("xx1", part.at[:, 0, :, pl.ds(0, sr)])
        all_sent("yy", yy)
    all_sent("zz", zout)
    for i, (ref, at) in enumerate(moved):
        all_sent(f"w{i}", at_rows(ref, at))
    all_sent("t0", mate_sum)
    all_sent("t1", far_sums)
    all_sent("t2", others)


def layer(tokens, ids, probs, wg, wu, wd, sg, su, sd):
    rows, dim = tokens.shape
    hid = sg.shape[0]
    rw = dim - GR + GR // NY
    any_spec = pl.BlockSpec(memory_space=pl.ANY)
    dma = pltpu.SemaphoreType.DMA
    last = (2 * NY, rows // 2, dim // NY)
    return pl.pallas_call(
        kernel,
        out_shape=jax.ShapeDtypeStruct((rows, dim), BF),
        in_specs=[any_spec] * 9,
        out_specs=pl.BlockSpec(memory_space=pltpu.VMEM),
        scratch_shapes=[
            pltpu.VMEM((NZ, 2, rows, dim), BF),
            pltpu.VMEM((NZ, 2, rows, dim), BF),
            pltpu.VMEM((NZ, NY - 1, 2, rows, max(GR // NY, 128)), BF),
            pltpu.VMEM((NZ, rows, rw), BF),
            pltpu.VMEM((2, NZ - 1, rows // 2, rw), BF),
            pltpu.VMEM((2, NZ - 1, rows // 2, rw), BF),
            pltpu.VMEM((4 * hid, dim), BF),
            pltpu.VMEM((2 * hid, dim), BF),
            pltpu.VMEM((2 * hid, dim), BF),
            pltpu.VMEM((hid, dim), BF),
            pltpu.VMEM(ids.shape, jnp.int32),
            pltpu.VMEM(probs.shape, F32),
            pltpu.VMEM((8, NZ * 2 * rows), F32),
            pltpu.VMEM((4 * rows, 2 * hid), BF),
            pltpu.VMEM((rows, dim), F32),
            pltpu.VMEM(last, BF),
            pltpu.VMEM(last, BF),
            pltpu.VMEM(last[1:], BF),
            pltpu.VMEM(last, BF),
            dma((9,)), dma((14,)), dma((3,)), dma((NZ, 2)), dma((NZ,)), dma((NZ,)),
            dma((NZ,)), dma((NZ, 2)), dma((2, NZ - 1, 2)), dma((2,)), dma((1,)),
        ],
        compiler_params=pltpu.CompilerParams(
            collective_id=0, has_side_effects=True, vmem_limit_bytes=62 * 1024 * 1024
        ),
    )(tokens, ids, probs, wg, wu, wd, sg, su, sd)


def body(tokens, expert_ids, gate_probs, w_gate, w_up, w_down, shared_gate, shared_up, shared_down):
    dim = tokens.shape[1]
    stacked = lambda w: jnp.swapaxes(w, 1, 2).reshape(-1, dim)
    return layer(
        tokens, expert_ids.T, gate_probs.T, stacked(w_gate), stacked(w_up), w_down.reshape(-1, dim),
        shared_gate.T, shared_up.T, shared_down,
    )


def solution(mesh):
    torus = Mesh(mesh.devices.reshape(NZ, 2, 2, 4, 2), ("z", "xl", "c", "y", "xh"))
    e, t = ("z", "xl", "c"), ("y", "xh")
    return jax.shard_map(
        body,
        mesh=torus,
        in_specs=(
            P(e, None), P(), P(),
            P(e, None, t), P(e, None, t), P(e, t, None),
            P(None, t), P(None, t), P(t, None),
        ),
        out_specs=P(e, None),
        check_vma=False,
    )
```

```python
import jax
import jax.numpy as jnp
from jax import lax
from jax.experimental import pallas as pl
from jax.experimental.pallas import tpu as pltpu
from jax.sharding import Mesh
from jax.sharding import PartitionSpec as P

MESH = pl.DeviceIdType.MESH
NZ, NY = 8, 4
OFFSETS = (0, -1, 1, -2, 2, -3, 3, 4)
SLOT = {d % NZ: s for s, d in enumerate(OFFSETS)}
BF, F32 = jnp.bfloat16, jnp.float32
GA, GR = 512, 512
DC = 512
NT_DIMS = (((1,), (1,)), ((), ()))


def kernel(
    tokens, ids, probs, wg, wu, wd, sg, su, sd, out,
    gath, part, yy, xx, zin, zout, wguv, wdv, sguv, sdv, idv, prv, wsc, hbuf, sbuf,
    tsb, tsi, fin, agi,
    loc_sem, snd_sem, wt_sem, ag_sem, ax_sem, ya_sem, yr_sem, xx_sem, zin_sem, ts_sem, ta_sem,
):
    z, xl, c = lax.axis_index("z"), lax.axis_index("xl"), lax.axis_index("c")
    y, xh = lax.axis_index("y"), lax.axis_index("xh")
    rows, dim = tokens.shape
    half, quarter = rows // 2, rows // 4
    hid = wg.shape[0]
    width = hid // 2
    sa, sr = GA // NY, GR // NY
    ca, cr = dim - GA, dim - GR
    aw, rw = ca + sa, cr + sr
    zup, zdn = {"z": lax.rem(z + 1, NZ)}, {"z": lax.rem(z + NZ - 1, NZ)}
    xup = {"xl": 1 - xl, "xh": lax.rem(xh + xl, 2)}
    xdn = {"xl": 1 - xl, "xh": lax.rem(xh + 1 - xl, 2)}
    mate = {"c": 1 - c}
    yat = [lax.rem(y + i, NY) for i in range(NY)]
    peers = [(yat[i], lax.rem(xh + j, 2), i, j) for i in range(NY) for j in (0, 1)][1:]
    other = 1 - xl

    local = []

    def load(src, dst, common=None, size=0):
        sem = loc_sem.at[len(local)]
        if size:
            pltpu.make_async_copy(src.at[:, pl.ds(0, common)], dst.at[:, pl.ds(0, common)], sem).start()
            for i in range(NY):
                at = pl.multiple_of(common + yat[i] * size, 128)
                pltpu.make_async_copy(
                    src.at[:, pl.ds(at, size)], dst.at[:, pl.ds(common + i * size, size)], sem
                ).start()
        else:
            pltpu.make_async_copy(src, dst, sem).start()
        local.append(pltpu.make_async_copy(src, dst, sem))
        return local[-1:]

    def at_rows(ref, first):
        return ref.at[pl.ds(first, hid)]

    tok_cp = load(tokens, gath.at[0, xl], ca, sa)
    rt_cp = (
        load(wg, at_rows(wguv, 0), ca, sa)
        + load(wu, at_rows(wguv, hid), ca, sa)
        + load(wd, at_rows(wdv, 0), cr, sr)
    )
    id_cp = load(ids, idv) + load(probs, prv)
    sh_cp = (
        load(sg, at_rows(sguv, 0), ca, sa)
        + load(su, at_rows(sguv, hid), ca, sa)
        + load(sd, sdv, cr, sr)
    )

    barrier = pltpu.get_barrier_semaphore()
    greeted = [zup, zdn, xup, xdn, mate] + [{"y": yp} for yp in yat[1:]]
    for dev in greeted:
        pl.semaphore_signal(barrier, inc=1, device_id=dev, device_id_type=MESH)
    with jax.named_scope("barrier"):
        pl.semaphore_wait(barrier, len(greeted))

    kinds = {}

    def send(kind, src, dst, sem, dev):
        pltpu.make_async_remote_copy(
            src_ref=src, dst_ref=dst, send_sem=snd_sem.at[kinds.setdefault(kind, len(kinds))],
            recv_sem=sem, device_id=dev, device_id_type=MESH,
        ).start()

    def all_sent(kind, whole):
        pltpu.make_async_remote_copy(
            src_ref=whole, dst_ref=whole, send_sem=snd_sem.at[kinds[kind]], recv_sem=snd_sem.at[0],
            device_id=mate, device_id_type=MESH,
        ).wait_send()

    def arrive(dst, sem):
        pltpu.make_async_remote_copy(
            src_ref=dst, dst_ref=dst, send_sem=snd_sem.at[0], recv_sem=sem,
            device_id=mate, device_id_type=MESH,
        ).wait_recv()

    def slots(k):
        return (0,) if k == 0 else (7,) if k == 4 else (2 * k - 1, 2 * k)

    def unit(slot, b, h):
        return gath.at[slot, b, pl.ds(h * half, half), pl.ds(0, aw)]

    def hop(offset, h, up):
        nxt = SLOT[(offset - 1 if up else offset + 1) % NZ]
        send("z", unit(SLOT[offset % NZ], xl, h), unit(nxt, xl, h), ag_sem.at[nxt, h], zup if up else zdn)

    def across(slot, h):
        send("x", unit(slot, xl, h), unit(slot, xl, h), ax_sem.at[slot], xup if h == 0 else xdn)

    def gather_z(k):
        for h in (0, 1):
            for up in (True, False):
                if k == 4 and up != (h == 0):
                    continue
                offset = -k if up else k
                slot = SLOT[offset % NZ]
                arrive(unit(slot, xl, h), ag_sem.at[slot, h])
                if k < 3 or (k == 3 and up == (h == 0)):
                    hop(offset, h, up)
                across(slot, h)

    def piece(slot, i, n=1):
        blocks = pl.ds(other, 1) if slot == 0 else pl.ds(0, 2)
        return gath.at[slot, blocks, :, pl.ds(ca + i * sa, n * sa)]

    def gather_x(k):
        for slot in slots(k):
            arrive(gath.at[slot, other, :, pl.ds(0, aw)], ax_sem.at[slot])
            for i in range(1, NY if GA else 1):
                send("y" if slot else "y0", piece(slot, 0), piece(slot, NY - i), ya_sem.at[slot], {"y": yat[i]})

    def gather_y(k):
        for slot in slots(k) if GA else ():
            arrive(piece(slot, 1, NY - 1), ya_sem.at[slot])

    def ffn(x, gu_ref, d_ref, scales, write):
        m = x.shape[0]
        n = d_ref.shape[0]
        hs = []
        for first in range(0, n, hid):
            gu = lax.dot_general(
                gu_ref[2 * first : 2 * (first + hid)], x, NT_DIMS, preferred_element_type=F32
            )
            for at in range(0, hid, width):
                g, u = gu[at : at + width], gu[hid + at : hid + at + width]
                h = g / (1.0 + jnp.exp(-g)) * u
                hs.append(h if scales is None else h * scales[len(hs)])
        hbuf[pl.ds(0, m), pl.ds(0, n)] = jnp.concatenate(hs, axis=0).T.astype(BF)
        for lo in range(0, dim, DC):
            cols = pl.ds(lo, DC)
            write(cols, jnp.dot(hbuf[pl.ds(0, m), pl.ds(0, n)], d_ref[:, cols], preferred_element_type=F32))

    def weigh():
        group, pair = 4 * rows, 2 * rows
        lane = lax.broadcasted_iota(jnp.int32, (8, pair), 1)
        for slot, offset in enumerate(OFFSETS):
            gz = lax.rem(z + offset + NZ, NZ)
            lanes = pl.ds(pl.multiple_of(gz * group, group), group)
            for j in range(4):
                expert = (z * 4 + xl * 2 + (c if j < 2 else 1 - c)) * 2 + j % 2
                row = jnp.sum(jnp.where(idv[:, lanes] == expert, prv[:, lanes], 0.0), axis=0, keepdims=True)
                lo, hi = (jnp.broadcast_to(row[:, at : at + pair], (8, pair)) for at in (0, pair))
                even = jnp.where(lane < rows, lo, pltpu.roll(hi, rows, 1))
                odd = jnp.where(lane < rows, pltpu.roll(lo, rows, 1), hi)
                wsc[j : j + 1, slot * pair : (slot + 1) * pair] = jnp.where(c == 0, even, odd)[0:1]

    def compute(k):
        ss = slots(k)
        s0, ns = ss[0], len(ss)
        pair = 2 * rows
        scales = [wsc[j : j + 1, s0 * pair : (s0 + ns) * pair] for j in range(4)]

        def write(cols, p):
            part[pl.ds(s0, ns), :, :, cols] = p.astype(BF).reshape(ns, 2, rows, DC)

        ffn(gath[pl.ds(s0, ns)].reshape(ns * pair, dim), wguv, wdv, scales, write)
        if k == 0:
            part[0, xl] = (part[0, xl].astype(F32) + sbuf[...]).astype(BF)

    sides = ((0, xup), (1, xdn))

    def x_send(slot, h, dev, which):
        r, cols = pl.ds(h * half, half), bounds[which]
        send(
            f"xx{which}", part.at[slot, other, r, cols], xx.at[slot, r, cols],
            xx_sem.at[slot, h, which], dev,
        )

    bounds = (pl.ds(0, cr), pl.ds(cr, sr))

    def swap_y(k):
        for slot in slots(k):
            for i in range(1, NY):
                send(
                    "yy", part.at[slot, :, :, pl.ds(cr + i * sr, sr)], yy.at[slot, NY - i - 1],
                    yr_sem.at[slot], {"y": yat[i]},
                )
        for slot in slots(k):
            for h, dev in sides:
                x_send(slot, h, dev, 0)

    def sliced(slot, b, r):
        v = part[slot, b, r, cr:rw].astype(F32)
        for i in range(NY - 1):
            v = v + yy[slot, i, b, r].astype(F32)
        return v

    def swap_x(k):
        for slot in slots(k):
            arrive(yy.at[slot], yr_sem.at[slot])
            part[slot, other, :, cr:rw] = sliced(slot, other, slice(None)).astype(BF)
            for h, dev in sides:
                x_send(slot, h, dev, 1)

    def ring_step(s, which, r_in, r_full, sem, h, up):
        slot = SLOT[(-s if up else s) % NZ]
        cols = bounds[which]
        v = xx[slot, r_full, cols].astype(F32)
        v = v + (sliced(slot, xl, r_full) if which else part[slot, xl, r_full, cols].astype(F32))
        if s > 1:
            arrive(zin.at[h, s - 2, r_in, cols], sem(s - 2))
            v = v + zin[h, s - 2, r_in, cols].astype(F32)
        if s == NZ:
            return v.astype(BF)
        zout[h, s - 1, r_in, cols] = v.astype(BF)
        send(
            f"zz{which}", zout.at[h, s - 1, r_in, cols], zin.at[h, s - 1, r_in, cols],
            sem(s - 1), zup if up else zdn,
        )

    directions = ((0, True), (1, False))

    def ring(s):
        for h, up in directions:
            slot = SLOT[(-s if up else s) % NZ]
            x_at = xx.at[slot, pl.ds(h * half, half), bounds[0]]
            arrive(x_at, xx_sem.at[slot, h, 0])
        for q in (0, 1):
            for h, up in directions:
                v = ring_step(
                    s, 0, pl.ds(q * quarter, quarter), pl.ds(h * half + q * quarter, quarter),
                    lambda i: zin_sem.at[h, i, q], h, up,
                )
                for i in range(NY if s == NZ else 0):
                    tsb[2 * i + h, q * quarter : (q + 1) * quarter, 0:cw] = v[:, i * cw : (i + 1) * cw]

    def ring_slice(s):
        for h, up in directions:
            slot = SLOT[(-s if up else s) % NZ]
            full = pl.ds(h * half, half)
            arrive(xx.at[slot, full, bounds[1]], xx_sem.at[slot, h, 1])
            v = ring_step(s, 1, pl.ds(0, half), full, lambda i: zin_sem.at[h, i, 2], h, up)
            if s == NZ:
                tsb[2 * y + h, :, cw : cw + sr] = v

    cw = cr // NY

    def tensor_send(far):
        n = cw if far else cw + sr
        for yp, xp, i, j in peers:
            if far == min(i, 1):
                send(
                    f"t{far}", tsb.at[2 * yp + xp, :, pl.ds(0, n)],
                    tsi.at[2 * ((NY - i) % NY) + j, :, pl.ds(0, n)],
                    ts_sem.at[far], {"y": yp, "xh": xp},
                )

    for cp in tok_cp:
        cp.wait()
    for h in (0, 1):
        hop(0, h, True)
        hop(0, h, False)
        across(0, h)
    for cp in rt_cp:
        cp.wait()
    moved = ((wguv, 2 * hid), (wdv, hid))
    for i, (ref, n) in enumerate(moved):
        send(f"w{i}", ref.at[pl.ds(0, n)], ref.at[pl.ds(n, n)], wt_sem.at[i], mate)
    for cp in id_cp + sh_cp:
        cp.wait()

    def write_shared(cols, p):
        sbuf[:, cols] = p

    with jax.named_scope("shared"):
        ffn(gath[0, xl], sguv, sdv, None, write_shared)
    with jax.named_scope("weigh"):
        weigh()

    def weights():
        for i, (ref, n) in enumerate(moved):
            arrive(ref.at[pl.ds(n, n)], wt_sem.at[i])

    with jax.named_scope("s00_gz1"):
        gather_z(1)
    with jax.named_scope("s01_gx0"):
        gather_x(0)
    with jax.named_scope("s02_gz2"):
        gather_z(2)
    with jax.named_scope("s03_gx1"):
        gather_x(1)
    with jax.named_scope("s04_gy0"):
        gather_y(0)
    with jax.named_scope("s05_w"):
        weights()
    with jax.named_scope("s06_c0"):
        compute(0)
    with jax.named_scope("s07_gz3"):
        gather_z(3)
    with jax.named_scope("s08_gx2"):
        gather_x(2)
    with jax.named_scope("s09_gy1"):
        gather_y(1)
    with jax.named_scope("s10_c1"):
        compute(1)
    with jax.named_scope("s11_gz4"):
        gather_z(4)
    with jax.named_scope("s12_sy1"):
        swap_y(1)
    with jax.named_scope("s13_gx3"):
        gather_x(3)
    with jax.named_scope("s14_gy2"):
        gather_y(2)
    with jax.named_scope("s15_c2"):
        compute(2)
    with jax.named_scope("s16_sy2"):
        swap_y(2)
    with jax.named_scope("s17_sx1"):
        swap_x(1)
    with jax.named_scope("s18_gx4"):
        gather_x(4)
    with jax.named_scope("s19_gy3"):
        gather_y(3)
    with jax.named_scope("s20_r1"):
        ring(1)
    with jax.named_scope("s21_c3"):
        compute(3)
    with jax.named_scope("s22_sy3"):
        swap_y(3)
    with jax.named_scope("s23_sx2"):
        swap_x(2)
    with jax.named_scope("s24_gy4"):
        gather_y(4)
    with jax.named_scope("s25_r2"):
        ring(2)
    with jax.named_scope("s26_q1"):
        ring_slice(1)
    with jax.named_scope("s27_c4"):
        compute(4)
    with jax.named_scope("s28_sy4"):
        swap_y(4)
    with jax.named_scope("s29_sx3"):
        swap_x(3)
    with jax.named_scope("s30_r3"):
        ring(3)
    with jax.named_scope("s31_q2"):
        ring_slice(2)
    with jax.named_scope("s32_sx4"):
        swap_x(4)
    with jax.named_scope("s33_q3"):
        ring_slice(3)
    with jax.named_scope("s34_r4"):
        ring(4)
    with jax.named_scope("s35_q4"):
        ring_slice(4)
    with jax.named_scope("s36_sy0"):
        swap_y(0)
    with jax.named_scope("s37_r5"):
        ring(5)
    with jax.named_scope("s38_q5"):
        ring_slice(5)
    with jax.named_scope("s39_sx0"):
        swap_x(0)
    with jax.named_scope("s40_r6"):
        ring(6)
    with jax.named_scope("s41_q6"):
        ring_slice(6)
    with jax.named_scope("s42_r7"):
        ring(7)
    with jax.named_scope("s43_q7"):
        ring_slice(7)
    with jax.named_scope("s44_r8"):
        ring(8)
    with jax.named_scope("s45_t"):
        tensor_send(1)
    with jax.named_scope("s46_q8"):
        ring_slice(8)
    me = 2 * y + xh
    with jax.named_scope("tensor_sum"):
        tensor_send(0)
        mate_sum, far_sums = tsi.at[1, :, pl.ds(0, cw + sr)], tsi.at[pl.ds(2, 6), :, pl.ds(0, cw)]
        arrive(mate_sum, ts_sem.at[0])
        acc = tsb[me, :, 0:cw].astype(F32) + tsi[1, :, 0:cw].astype(F32)
        fin[:, cw : cw + sr] = (
            tsb[me, :, cw : cw + sr].astype(F32) + tsi[1, :, cw : cw + sr].astype(F32)
        ).astype(BF)
        arrive(far_sums, ts_sem.at[1])
        for i in range(2, 8):
            acc = acc + tsi[i, :, 0:cw].astype(F32)
        fin[:, 0:cw] = acc.astype(BF)
    with jax.named_scope("tensor_all"):
        for yp, xp, i, j in peers:
            send("t2", fin, agi.at[me], ta_sem.at[0], {"y": yp, "xh": xp})
        agi[me] = fin[...]
        others = agi.at[pl.ds(0, 7)]
        arrive(others, ta_sem.at[0])
        for i in range(NY):
            for j in (0, 1):
                r = pl.ds(j * half, half)
                out[r, i * cw : (i + 1) * cw] = agi[2 * i + j, :, 0:cw]
                out[r, cr + i * sr : cr + (i + 1) * sr] = agi[2 * i + j, :, cw : cw + sr]
    all_sent("z", gath.at[pl.ds(0, 7), 0, :, pl.ds(0, aw)])
    all_sent("x", gath.at[:, 0, :, pl.ds(0, aw)])
    if GA:
        all_sent("y", gath.at[pl.ds(0, 7), :, :, pl.ds(0, 3 * sa)])
        all_sent("y0", gath.at[0, 0, :, pl.ds(0, 3 * sa)])
    all_sent("xx0", part.at[:, 0, :, pl.ds(0, cr)])
    all_sent("xx1", part.at[:, 0, :, pl.ds(0, sr)])
    all_sent("yy", yy)
    all_sent("zz0", zout.at[:, :, :, bounds[0]])
    all_sent("zz1", zout.at[:, :, :, bounds[1]])
    for i, (ref, n) in enumerate(moved):
        all_sent(f"w{i}", ref.at[pl.ds(0, n)])
    all_sent("t0", mate_sum)
    all_sent("t1", far_sums)
    all_sent("t2", others)


def layer(tokens, ids, probs, wg, wu, wd, sg, su, sd):
    rows, dim = tokens.shape
    hid = sg.shape[0]
    rw = dim - GR + GR // NY
    any_spec = pl.BlockSpec(memory_space=pl.ANY)
    dma = pltpu.SemaphoreType.DMA
    last = (2 * NY, rows // 2, dim // NY)
    return pl.pallas_call(
        kernel,
        out_shape=jax.ShapeDtypeStruct((rows, dim), BF),
        in_specs=[any_spec] * 9,
        out_specs=pl.BlockSpec(memory_space=pltpu.VMEM),
        scratch_shapes=[
            pltpu.VMEM((NZ, 2, rows, dim), BF),
            pltpu.VMEM((NZ, 2, rows, dim), BF),
            pltpu.VMEM((NZ, NY - 1, 2, rows, max(GR // NY, 128)), BF),
            pltpu.VMEM((NZ, rows, rw), BF),
            pltpu.VMEM((2, NZ - 1, rows // 2, rw), BF),
            pltpu.VMEM((2, NZ - 1, rows // 2, rw), BF),
            pltpu.VMEM((4 * hid, dim), BF),
            pltpu.VMEM((2 * hid, dim), BF),
            pltpu.VMEM((2 * hid, dim), BF),
            pltpu.VMEM((hid, dim), BF),
            pltpu.VMEM(ids.shape, jnp.int32),
            pltpu.VMEM(probs.shape, F32),
            pltpu.VMEM((8, NZ * 2 * rows), F32),
            pltpu.VMEM((4 * rows, 2 * hid), BF),
            pltpu.VMEM((rows, dim), F32),
            pltpu.VMEM(last, BF),
            pltpu.VMEM(last, BF),
            pltpu.VMEM(last[1:], BF),
            pltpu.VMEM(last, BF),
            dma((9,)), dma((15,)), dma((2,)), dma((NZ, 2)), dma((NZ,)), dma((NZ,)),
            dma((NZ,)), dma((NZ, 2, 2)), dma((2, NZ - 1, 3)), dma((2,)), dma((1,)),
        ],
        compiler_params=pltpu.CompilerParams(
            collective_id=0, has_side_effects=True, vmem_limit_bytes=62 * 1024 * 1024
        ),
    )(tokens, ids, probs, wg, wu, wd, sg, su, sd)


def body(tokens, expert_ids, gate_probs, w_gate, w_up, w_down, shared_gate, shared_up, shared_down):
    dim = tokens.shape[1]
    stacked = lambda w: jnp.swapaxes(w, 1, 2).reshape(-1, dim)
    return layer(
        tokens, expert_ids.T, gate_probs.T, stacked(w_gate), stacked(w_up), w_down.reshape(-1, dim),
        shared_gate.T, shared_up.T, shared_down,
    )


def solution(mesh):
    torus = Mesh(mesh.devices.reshape(NZ, 2, 2, 4, 2), ("z", "xl", "c", "y", "xh"))
    e, t = ("z", "xl", "c"), ("y", "xh")
    return jax.shard_map(
        body,
        mesh=torus,
        in_specs=(
            P(e, None), P(), P(),
            P(e, None, t), P(e, None, t), P(e, t, None),
            P(None, t), P(None, t), P(t, None),
        ),
        out_specs=P(e, None),
        check_vma=False,
    )
```

```python
import jax
import jax.numpy as jnp
from jax import lax
from jax.experimental import pallas as pl
from jax.experimental.pallas import tpu as pltpu
from jax.sharding import Mesh
from jax.sharding import PartitionSpec as P

MESH = pl.DeviceIdType.MESH
NZ, NY = 8, 4
OFFSETS = (0, -1, 1, -2, 2, -3, 3, 4)
SLOT = {d % NZ: s for s, d in enumerate(OFFSETS)}
BF, F32 = jnp.bfloat16, jnp.float32
GA, GR = 512, 512
DC = 512
NP = 2
NT_DIMS = (((1,), (1,)), ((), ()))


def kernel(
    tokens, ids, probs, wg, wu, wd, sg, su, sd, out,
    gath, part, yy, xx, zin, zout, wguv, wdv, sguv, sdv, idv, prv, wsc, hbuf, sbuf,
    tsb, tsi, fin, agi,
    loc_sem, snd_sem, wt_sem, ag_sem, ax_sem, ya_sem, yr_sem, xx_sem, zin_sem, ts_sem, ta_sem,
):
    z, xl, c = lax.axis_index("z"), lax.axis_index("xl"), lax.axis_index("c")
    y, xh = lax.axis_index("y"), lax.axis_index("xh")
    rows, dim = tokens.shape
    half, quarter = rows // 2, rows // 4
    hid = wg.shape[0]
    width = hid // 2
    sa, sr = GA // NY, GR // NY
    ca, cr = dim - GA, dim - GR
    aw, rw = ca + sa, cr + sr
    zup, zdn = {"z": lax.rem(z + 1, NZ)}, {"z": lax.rem(z + NZ - 1, NZ)}
    xup = {"xl": 1 - xl, "xh": lax.rem(xh + xl, 2)}
    xdn = {"xl": 1 - xl, "xh": lax.rem(xh + 1 - xl, 2)}
    mate = {"c": 1 - c}
    yat = [lax.rem(y + i, NY) for i in range(NY)]
    peers = [(yat[i], lax.rem(xh + j, 2), i, j) for i in range(NY) for j in (0, 1)][1:]
    other = 1 - xl

    local = []

    def load(src, dst, common=None, size=0):
        sem = loc_sem.at[len(local)]
        if size:
            pltpu.make_async_copy(src.at[:, pl.ds(0, common)], dst.at[:, pl.ds(0, common)], sem).start()
            for i in range(NY):
                at = pl.multiple_of(common + yat[i] * size, 128)
                pltpu.make_async_copy(
                    src.at[:, pl.ds(at, size)], dst.at[:, pl.ds(common + i * size, size)], sem
                ).start()
        else:
            pltpu.make_async_copy(src, dst, sem).start()
        local.append(pltpu.make_async_copy(src, dst, sem))
        return local[-1:]

    def at_rows(ref, first):
        return ref.at[pl.ds(first, hid)]

    tok_cp = load(tokens, gath.at[0, xl], ca, sa)
    rt_cp = (
        load(wg, at_rows(wguv, 0), ca, sa)
        + load(wu, at_rows(wguv, hid), ca, sa)
        + load(wd, at_rows(wdv, 0), cr, sr)
    )
    id_cp = load(ids, idv) + load(probs, prv)
    sh_cp = (
        load(sg, at_rows(sguv, 0), ca, sa)
        + load(su, at_rows(sguv, hid), ca, sa)
        + load(sd, sdv, cr, sr)
    )

    barrier = pltpu.get_barrier_semaphore()
    greeted = [zup, zdn, xup, xdn, mate] + [{"y": yp} for yp in yat[1:]]
    for dev in greeted:
        pl.semaphore_signal(barrier, inc=1, device_id=dev, device_id_type=MESH)
    with jax.named_scope("barrier"):
        pl.semaphore_wait(barrier, len(greeted))

    kinds = {}

    def send(kind, src, dst, sem, dev):
        pltpu.make_async_remote_copy(
            src_ref=src, dst_ref=dst, send_sem=snd_sem.at[kinds.setdefault(kind, len(kinds))],
            recv_sem=sem, device_id=dev, device_id_type=MESH,
        ).start()

    def all_sent(kind, whole):
        pltpu.make_async_remote_copy(
            src_ref=whole, dst_ref=whole, send_sem=snd_sem.at[kinds[kind]], recv_sem=snd_sem.at[0],
            device_id=mate, device_id_type=MESH,
        ).wait_send()

    def arrive(dst, sem):
        pltpu.make_async_remote_copy(
            src_ref=dst, dst_ref=dst, send_sem=snd_sem.at[0], recv_sem=sem,
            device_id=mate, device_id_type=MESH,
        ).wait_recv()

    def slots(k):
        return (0,) if k == 0 else (7,) if k == 4 else (2 * k - 1, 2 * k)

    def unit(slot, b, h):
        return gath.at[slot, b, pl.ds(h * half, half), pl.ds(0, aw)]

    def hop(offset, h, up):
        nxt = SLOT[(offset - 1 if up else offset + 1) % NZ]
        send("z", unit(SLOT[offset % NZ], xl, h), unit(nxt, xl, h), ag_sem.at[nxt, h], zup if up else zdn)

    def across(slot, h):
        send("x", unit(slot, xl, h), unit(slot, xl, h), ax_sem.at[slot], xup if h == 0 else xdn)

    def gather_z(k):
        for h in (0, 1):
            for up in (True, False):
                if k == 4 and up != (h == 0):
                    continue
                offset = -k if up else k
                slot = SLOT[offset % NZ]
                arrive(unit(slot, xl, h), ag_sem.at[slot, h])
                if k < 3 or (k == 3 and up == (h == 0)):
                    hop(offset, h, up)
                across(slot, h)

    def piece(slot, i, n=1):
        blocks = pl.ds(other, 1) if slot == 0 else pl.ds(0, 2)
        return gath.at[slot, blocks, :, pl.ds(ca + i * sa, n * sa)]

    def gather_x(k):
        for slot in slots(k):
            arrive(gath.at[slot, other, :, pl.ds(0, aw)], ax_sem.at[slot])
            for i in range(1, NY if GA else 1):
                send("y" if slot else "y0", piece(slot, 0), piece(slot, NY - i), ya_sem.at[slot], {"y": yat[i]})

    def gather_y(k):
        for slot in slots(k) if GA else ():
            arrive(piece(slot, 1, NY - 1), ya_sem.at[slot])

    def ffn(x, gu_ref, d_ref, scales, write):
        m = x.shape[0]
        n = d_ref.shape[0]
        hs = []
        for first in range(0, n, hid):
            gu = lax.dot_general(
                gu_ref[2 * first : 2 * (first + hid)], x, NT_DIMS, preferred_element_type=F32
            )
            for at in range(0, hid, width):
                g, u = gu[at : at + width], gu[hid + at : hid + at + width]
                h = g / (1.0 + jnp.exp(-g)) * u
                hs.append(h if scales is None else h * scales[len(hs)])
        hbuf[pl.ds(0, m), pl.ds(0, n)] = jnp.concatenate(hs, axis=0).T.astype(BF)
        for lo in range(0, dim, DC):
            cols = pl.ds(lo, DC)
            write(cols, jnp.dot(hbuf[pl.ds(0, m), pl.ds(0, n)], d_ref[:, cols], preferred_element_type=F32))

    def weigh():
        group, pair = 4 * rows, 2 * rows
        lane = lax.broadcasted_iota(jnp.int32, (8, pair), 1)
        for slot, offset in enumerate(OFFSETS):
            gz = lax.rem(z + offset + NZ, NZ)
            lanes = pl.ds(pl.multiple_of(gz * group, group), group)
            for j in range(4):
                expert = (z * 4 + xl * 2 + (c if j < 2 else 1 - c)) * 2 + j % 2
                row = jnp.sum(jnp.where(idv[:, lanes] == expert, prv[:, lanes], 0.0), axis=0, keepdims=True)
                lo, hi = (jnp.broadcast_to(row[:, at : at + pair], (8, pair)) for at in (0, pair))
                even = jnp.where(lane < rows, lo, pltpu.roll(hi, rows, 1))
                odd = jnp.where(lane < rows, pltpu.roll(lo, rows, 1), hi)
                wsc[j : j + 1, slot * pair : (slot + 1) * pair] = jnp.where(c == 0, even, odd)[0:1]

    def compute(k):
        ss = slots(k)
        s0, ns = ss[0], len(ss)
        pair = 2 * rows
        scales = [wsc[j : j + 1, s0 * pair : (s0 + ns) * pair] for j in range(4)]

        def write(cols, p):
            part[pl.ds(s0, ns), :, :, cols] = p.astype(BF).reshape(ns, 2, rows, DC)

        ffn(gath[pl.ds(s0, ns)].reshape(ns * pair, dim), wguv, wdv, scales, write)
        if k == 0:
            part[0, xl] = (part[0, xl].astype(F32) + sbuf[...]).astype(BF)

    sides = ((0, xup), (1, xdn))

    def x_send(slot, h, dev, which):
        r, cols = pl.ds(h * half, half), bounds[which]
        send(
            f"xx{which}", part.at[slot, other, r, cols], xx.at[slot, r, cols],
            xx_sem.at[slot, h, which], dev,
        )

    bounds = (pl.ds(0, cr), pl.ds(cr, sr))

    def swap_y(k):
        for slot in slots(k):
            for i in range(1, NY):
                send(
                    "yy", part.at[slot, :, :, pl.ds(cr + i * sr, sr)], yy.at[slot, NY - i - 1],
                    yr_sem.at[slot], {"y": yat[i]},
                )
        swap_common(k, True)

    def swap_common(k, soon):
        for slot in slots(k):
            for h, dev in sides:
                if soon == (k in (0, 4) or (h == 0) == (OFFSETS[slot] < 0)):
                    x_send(slot, h, dev, 0)

    def swap_late(k):
        swap_common(k, False)

    def sliced(slot, b, r):
        v = part[slot, b, r, cr:rw].astype(F32)
        for i in range(NY - 1):
            v = v + yy[slot, i, b, r].astype(F32)
        return v

    def swap_x(k):
        for slot in slots(k):
            arrive(yy.at[slot], yr_sem.at[slot])
            part[slot, other, :, cr:rw] = sliced(slot, other, slice(None)).astype(BF)
            for h, dev in sides:
                x_send(slot, h, dev, 1)

    def ring_step(s, which, cols, r_in, r_full, sem, h, up):
        slot = SLOT[(-s if up else s) % NZ]
        v = xx[slot, r_full, cols].astype(F32)
        v = v + (sliced(slot, xl, r_full) if which else part[slot, xl, r_full, cols].astype(F32))
        if s > 1:
            arrive(zin.at[h, s - 2, r_in, cols], sem(s - 2))
            v = v + zin[h, s - 2, r_in, cols].astype(F32)
        if s == NZ:
            return v.astype(BF)
        zout[h, s - 1, r_in, cols] = v.astype(BF)
        send(
            f"zz{which}", zout.at[h, s - 1, r_in, cols], zin.at[h, s - 1, r_in, cols],
            sem(s - 1), zup if up else zdn,
        )

    directions = ((0, True), (1, False))

    def ring(s):
        for h, up in directions:
            slot = SLOT[(-s if up else s) % NZ]
            x_at = xx.at[slot, pl.ds(h * half, half), bounds[0]]
            arrive(x_at, xx_sem.at[slot, h, 0])
        n = cr // NP
        for q, p in [(q, p) for q in (0, 1) for p in range(NP)]:
            for h, up in directions:
                v = ring_step(
                    s, 0, pl.ds(p * n, n), pl.ds(q * quarter, quarter),
                    pl.ds(h * half + q * quarter, quarter),
                    lambda i: zin_sem.at[h, i, q * NP + p], h, up,
                )
                for i in range(NY // NP if s == NZ else 0):
                    at = 2 * (p * NY // NP + i) + h
                    tsb[at, q * quarter : (q + 1) * quarter, 0:cw] = v[:, i * cw : (i + 1) * cw]

    def ring_slice(s):
        for h, up in directions:
            slot = SLOT[(-s if up else s) % NZ]
            full = pl.ds(h * half, half)
            arrive(xx.at[slot, full, bounds[1]], xx_sem.at[slot, h, 1])
            v = ring_step(s, 1, bounds[1], pl.ds(0, half), full, lambda i: zin_sem.at[h, i, 2 * NP], h, up)
            if s == NZ:
                tsb[2 * y + h, :, cw : cw + sr] = v

    cw = cr // NY

    def tensor_send(far):
        n = cw if far else cw + sr
        for yp, xp, i, j in peers:
            if far == min(i, 1):
                send(
                    f"t{far}", tsb.at[2 * yp + xp, :, pl.ds(0, n)],
                    tsi.at[2 * ((NY - i) % NY) + j, :, pl.ds(0, n)],
                    ts_sem.at[far], {"y": yp, "xh": xp},
                )

    for cp in tok_cp:
        cp.wait()
    for h in (0, 1):
        hop(0, h, True)
        hop(0, h, False)
        across(0, h)
    for cp in rt_cp:
        cp.wait()
    moved = ((wguv, 2 * hid), (wdv, hid))
    for i, (ref, n) in enumerate(moved):
        send(f"w{i}", ref.at[pl.ds(0, n)], ref.at[pl.ds(n, n)], wt_sem.at[i], mate)
    for cp in id_cp + sh_cp:
        cp.wait()

    def write_shared(cols, p):
        sbuf[:, cols] = p

    with jax.named_scope("shared"):
        ffn(gath[0, xl], sguv, sdv, None, write_shared)
    with jax.named_scope("weigh"):
        weigh()

    def weights():
        for i, (ref, n) in enumerate(moved):
            arrive(ref.at[pl.ds(n, n)], wt_sem.at[i])

    with jax.named_scope("s00_gz1"):
        gather_z(1)
    with jax.named_scope("s01_gx0"):
        gather_x(0)
    with jax.named_scope("s02_gz2"):
        gather_z(2)
    with jax.named_scope("s03_gx1"):
        gather_x(1)
    with jax.named_scope("s04_gy0"):
        gather_y(0)
    with jax.named_scope("s05_w"):
        weights()
    with jax.named_scope("s06_c0"):
        compute(0)
    with jax.named_scope("s07_gz3"):
        gather_z(3)
    with jax.named_scope("s08_gx2"):
        gather_x(2)
    with jax.named_scope("s09_gy1"):
        gather_y(1)
    with jax.named_scope("s10_c1"):
        compute(1)
    with jax.named_scope("s11_gz4"):
        gather_z(4)
    with jax.named_scope("s12_sy1"):
        swap_y(1)
    with jax.named_scope("s13_gx3"):
        gather_x(3)
    with jax.named_scope("s14_gy2"):
        gather_y(2)
    with jax.named_scope("s15_c2"):
        compute(2)
    with jax.named_scope("s16_sy2"):
        swap_y(2)
    with jax.named_scope("s17_sx1"):
        swap_x(1)
    with jax.named_scope("s18_gx4"):
        gather_x(4)
    with jax.named_scope("s19_gy3"):
        gather_y(3)
    with jax.named_scope("s20_r1"):
        ring(1)
    with jax.named_scope("s21_c3"):
        compute(3)
    with jax.named_scope("s22_sy3"):
        swap_y(3)
    with jax.named_scope("s23_sx2"):
        swap_x(2)
    with jax.named_scope("s24_gy4"):
        gather_y(4)
    with jax.named_scope("s25_r2"):
        ring(2)
    with jax.named_scope("s26_q1"):
        ring_slice(1)
    with jax.named_scope("s27_c4"):
        compute(4)
    with jax.named_scope("s28_sy4"):
        swap_y(4)
    with jax.named_scope("s29_sx3"):
        swap_x(3)
    with jax.named_scope("s30_r3"):
        ring(3)
    with jax.named_scope("s31_q2"):
        ring_slice(2)
    with jax.named_scope("s32_xl3"):
        swap_late(3)
    with jax.named_scope("s33_sx4"):
        swap_x(4)
    with jax.named_scope("s34_r4"):
        ring(4)
    with jax.named_scope("s35_q3"):
        ring_slice(3)
    with jax.named_scope("s36_xl2"):
        swap_late(2)
    with jax.named_scope("s37_r5"):
        ring(5)
    with jax.named_scope("s38_q4"):
        ring_slice(4)
    with jax.named_scope("s39_xl1"):
        swap_late(1)
    with jax.named_scope("s40_sy0"):
        swap_y(0)
    with jax.named_scope("s41_r6"):
        ring(6)
    with jax.named_scope("s42_q5"):
        ring_slice(5)
    with jax.named_scope("s43_sx0"):
        swap_x(0)
    with jax.named_scope("s44_r7"):
        ring(7)
    with jax.named_scope("s45_q6"):
        ring_slice(6)
    with jax.named_scope("s46_q7"):
        ring_slice(7)
    with jax.named_scope("s47_r8"):
        ring(8)
    with jax.named_scope("s48_t"):
        tensor_send(1)
    with jax.named_scope("s49_q8"):
        ring_slice(8)
    me = 2 * y + xh
    with jax.named_scope("tensor_sum"):
        tensor_send(0)
        mate_sum, far_sums = tsi.at[1, :, pl.ds(0, cw + sr)], tsi.at[pl.ds(2, 6), :, pl.ds(0, cw)]
        arrive(mate_sum, ts_sem.at[0])
        acc = tsb[me, :, 0:cw].astype(F32) + tsi[1, :, 0:cw].astype(F32)
        fin[:, cw : cw + sr] = (
            tsb[me, :, cw : cw + sr].astype(F32) + tsi[1, :, cw : cw + sr].astype(F32)
        ).astype(BF)
        arrive(far_sums, ts_sem.at[1])
        for i in range(2, 8):
            acc = acc + tsi[i, :, 0:cw].astype(F32)
        fin[:, 0:cw] = acc.astype(BF)
    with jax.named_scope("tensor_all"):
        for yp, xp, i, j in peers:
            send("t2", fin, agi.at[me], ta_sem.at[0], {"y": yp, "xh": xp})
        agi[me] = fin[...]
        others = agi.at[pl.ds(0, 7)]
        arrive(others, ta_sem.at[0])
        for i in range(NY):
            for j in (0, 1):
                r = pl.ds(j * half, half)
                out[r, i * cw : (i + 1) * cw] = agi[2 * i + j, :, 0:cw]
                out[r, cr + i * sr : cr + (i + 1) * sr] = agi[2 * i + j, :, cw : cw + sr]
    all_sent("z", gath.at[pl.ds(0, 7), 0, :, pl.ds(0, aw)])
    all_sent("x", gath.at[:, 0, :, pl.ds(0, aw)])
    if GA:
        all_sent("y", gath.at[pl.ds(0, 7), :, :, pl.ds(0, 3 * sa)])
        all_sent("y0", gath.at[0, 0, :, pl.ds(0, 3 * sa)])
    all_sent("xx0", part.at[:, 0, :, pl.ds(0, cr)])
    all_sent("xx1", part.at[:, 0, :, pl.ds(0, sr)])
    all_sent("yy", yy)
    all_sent("zz0", zout.at[:, :, :, bounds[0]])
    all_sent("zz1", zout.at[:, :, :, bounds[1]])
    for i, (ref, n) in enumerate(moved):
        all_sent(f"w{i}", ref.at[pl.ds(0, n)])
    all_sent("t0", mate_sum)
    all_sent("t1", far_sums)
    all_sent("t2", others)


def layer(tokens, ids, probs, wg, wu, wd, sg, su, sd):
    rows, dim = tokens.shape
    hid = sg.shape[0]
    rw = dim - GR + GR // NY
    any_spec = pl.BlockSpec(memory_space=pl.ANY)
    dma = pltpu.SemaphoreType.DMA
    last = (2 * NY, rows // 2, dim // NY)
    return pl.pallas_call(
        kernel,
        out_shape=jax.ShapeDtypeStruct((rows, dim), BF),
        in_specs=[any_spec] * 9,
        out_specs=pl.BlockSpec(memory_space=pltpu.VMEM),
        scratch_shapes=[
            pltpu.VMEM((NZ, 2, rows, dim), BF),
            pltpu.VMEM((NZ, 2, rows, dim), BF),
            pltpu.VMEM((NZ, NY - 1, 2, rows, max(GR // NY, 128)), BF),
            pltpu.VMEM((NZ, rows, rw), BF),
            pltpu.VMEM((2, NZ - 1, rows // 2, rw), BF),
            pltpu.VMEM((2, NZ - 1, rows // 2, rw), BF),
            pltpu.VMEM((4 * hid, dim), BF),
            pltpu.VMEM((2 * hid, dim), BF),
            pltpu.VMEM((2 * hid, dim), BF),
            pltpu.VMEM((hid, dim), BF),
            pltpu.VMEM(ids.shape, jnp.int32),
            pltpu.VMEM(probs.shape, F32),
            pltpu.VMEM((8, NZ * 2 * rows), F32),
            pltpu.VMEM((4 * rows, 2 * hid), BF),
            pltpu.VMEM((rows, dim), F32),
            pltpu.VMEM(last, BF),
            pltpu.VMEM(last, BF),
            pltpu.VMEM(last[1:], BF),
            pltpu.VMEM(last, BF),
            dma((9,)), dma((15,)), dma((2,)), dma((NZ, 2)), dma((NZ,)), dma((NZ,)),
            dma((NZ,)), dma((NZ, 2, 2)), dma((2, NZ - 1, 2 * NP + 1)), dma((2,)), dma((1,)),
        ],
        compiler_params=pltpu.CompilerParams(
            collective_id=0, has_side_effects=True, vmem_limit_bytes=62 * 1024 * 1024
        ),
    )(tokens, ids, probs, wg, wu, wd, sg, su, sd)


def body(tokens, expert_ids, gate_probs, w_gate, w_up, w_down, shared_gate, shared_up, shared_down):
    dim = tokens.shape[1]
    stacked = lambda w: jnp.swapaxes(w, 1, 2).reshape(-1, dim)
    return layer(
        tokens, expert_ids.T, gate_probs.T, stacked(w_gate), stacked(w_up), w_down.reshape(-1, dim),
        shared_gate.T, shared_up.T, shared_down,
    )


def solution(mesh):
    torus = Mesh(mesh.devices.reshape(NZ, 2, 2, 4, 2), ("z", "xl", "c", "y", "xh"))
    e, t = ("z", "xl", "c"), ("y", "xh")
    return jax.shard_map(
        body,
        mesh=torus,
        in_specs=(
            P(e, None), P(), P(),
            P(e, None, t), P(e, None, t), P(e, t, None),
            P(None, t), P(None, t), P(t, None),
        ),
        out_specs=P(e, None),
        check_vma=False,
    )
```

```python
import jax
import jax.numpy as jnp
from jax import lax
from jax.experimental import pallas as pl
from jax.experimental.pallas import tpu as pltpu
from jax.sharding import Mesh
from jax.sharding import PartitionSpec as P

MESH = pl.DeviceIdType.MESH
NZ, NY = 8, 4
OFFSETS = (0, -1, 1, -2, 2, -3, 3, 4)
SLOT = {d % NZ: s for s, d in enumerate(OFFSETS)}
BF, F32 = jnp.bfloat16, jnp.float32
GA, GR = 512, 512
DC = 512
NP = 2
NT_DIMS = (((1,), (1,)), ((), ()))


def kernel(
    tokens, ids, probs, wg, wu, wd, sg, su, sd, out,
    gath, part, yy, xx, zin, zout, wguv, wdv, sguv, sdv, idv, prv, wsc, hbuf, sbuf,
    tsb, tsi, fin, agi,
    loc_sem, snd_sem, wt_sem, ag_sem, ax_sem, ya_sem, yr_sem, xx_sem, zin_sem, ts_sem, ta_sem,
):
    z, xl, c = lax.axis_index("z"), lax.axis_index("xl"), lax.axis_index("c")
    y, xh = lax.axis_index("y"), lax.axis_index("xh")
    rows, dim = tokens.shape
    half, quarter = rows // 2, rows // 4
    hid = wg.shape[0]
    width = hid // 2
    sa, sr = GA // NY, GR // NY
    ca, cr = dim - GA, dim - GR
    aw, rw = ca + sa, cr + sr
    zup, zdn = {"z": lax.rem(z + 1, NZ)}, {"z": lax.rem(z + NZ - 1, NZ)}
    xup = {"xl": 1 - xl, "xh": lax.rem(xh + xl, 2)}
    xdn = {"xl": 1 - xl, "xh": lax.rem(xh + 1 - xl, 2)}
    mate = {"c": 1 - c}
    yat = [lax.rem(y + i, NY) for i in range(NY)]
    peers = [(yat[i], lax.rem(xh + j, 2), i, j) for i in range(NY) for j in (0, 1)][1:]
    other = 1 - xl

    local = []

    def load(src, dst, common=None, size=0):
        sem = loc_sem.at[len(local)]
        if size:
            pltpu.make_async_copy(src.at[:, pl.ds(0, common)], dst.at[:, pl.ds(0, common)], sem).start()
            for i in range(NY):
                at = pl.multiple_of(common + yat[i] * size, 128)
                pltpu.make_async_copy(
                    src.at[:, pl.ds(at, size)], dst.at[:, pl.ds(common + i * size, size)], sem
                ).start()
        else:
            pltpu.make_async_copy(src, dst, sem).start()
        local.append(pltpu.make_async_copy(src, dst, sem))
        return local[-1:]

    def at_rows(ref, first):
        return ref.at[pl.ds(first, hid)]

    tok_cp = load(tokens, gath.at[0, xl], ca, sa)
    rt_cp = (
        load(wg, at_rows(wguv, 0), ca, sa)
        + load(wu, at_rows(wguv, hid), ca, sa)
        + load(wd, at_rows(wdv, 0), cr, sr)
    )
    id_cp = load(ids, idv) + load(probs, prv)
    sh_cp = (
        load(sg, at_rows(sguv, 0), ca, sa)
        + load(su, at_rows(sguv, hid), ca, sa)
        + load(sd, sdv, cr, sr)
    )

    barrier = pltpu.get_barrier_semaphore()
    greeted = [zup, zdn, xup, xdn, mate] + [{"y": yp} for yp in yat[1:]]
    for dev in greeted:
        pl.semaphore_signal(barrier, inc=1, device_id=dev, device_id_type=MESH)
    with jax.named_scope("barrier"):
        pl.semaphore_wait(barrier, len(greeted))

    kinds = {}

    def send(kind, src, dst, sem, dev):
        pltpu.make_async_remote_copy(
            src_ref=src, dst_ref=dst, send_sem=snd_sem.at[kinds.setdefault(kind, len(kinds))],
            recv_sem=sem, device_id=dev, device_id_type=MESH,
        ).start()

    def all_sent(kind, whole):
        pltpu.make_async_remote_copy(
            src_ref=whole, dst_ref=whole, send_sem=snd_sem.at[kinds[kind]], recv_sem=snd_sem.at[0],
            device_id=mate, device_id_type=MESH,
        ).wait_send()

    def arrive(dst, sem):
        pltpu.make_async_remote_copy(
            src_ref=dst, dst_ref=dst, send_sem=snd_sem.at[0], recv_sem=sem,
            device_id=mate, device_id_type=MESH,
        ).wait_recv()

    def slots(k):
        return (0,) if k == 0 else (7,) if k == 4 else (2 * k - 1, 2 * k)

    def unit(slot, b, h):
        return gath.at[slot, b, pl.ds(h * half, half), pl.ds(0, aw)]

    def hop(offset, h, up):
        nxt = SLOT[(offset - 1 if up else offset + 1) % NZ]
        send("z", unit(SLOT[offset % NZ], xl, h), unit(nxt, xl, h), ag_sem.at[nxt, h], zup if up else zdn)

    def across(slot, h):
        send("x", unit(slot, xl, h), unit(slot, xl, h), ax_sem.at[slot], xup if h == 0 else xdn)

    def gather_z(k):
        for h in (0, 1):
            for up in (True, False):
                if k == 4 and up != (h == 0):
                    continue
                offset = -k if up else k
                slot = SLOT[offset % NZ]
                arrive(unit(slot, xl, h), ag_sem.at[slot, h])
                if k < 3 or (k == 3 and up == (h == 0)):
                    hop(offset, h, up)
                across(slot, h)

    def piece(slot, i, n=1):
        blocks = pl.ds(other, 1) if slot == 0 else pl.ds(0, 2)
        return gath.at[slot, blocks, :, pl.ds(ca + i * sa, n * sa)]

    def gather_x(k):
        for slot in slots(k):
            arrive(gath.at[slot, other, :, pl.ds(0, aw)], ax_sem.at[slot])
            for i in range(1, NY if GA else 1):
                send("y" if slot else "y0", piece(slot, 0), piece(slot, NY - i), ya_sem.at[slot], {"y": yat[i]})

    def gather_y(k):
        for slot in slots(k) if GA else ():
            arrive(piece(slot, 1, NY - 1), ya_sem.at[slot])

    def ffn(x, gu_ref, d_ref, scales, write):
        m = x.shape[0]
        n = d_ref.shape[0]
        hs = []
        for first in range(0, n, hid):
            gu = lax.dot_general(
                gu_ref[2 * first : 2 * (first + hid)], x, NT_DIMS, preferred_element_type=F32
            )
            for at in range(0, hid, width):
                g, u = gu[at : at + width], gu[hid + at : hid + at + width]
                h = g / (1.0 + jnp.exp(-g)) * u
                hs.append(h if scales is None else h * scales[len(hs)])
        hbuf[pl.ds(0, m), pl.ds(0, n)] = jnp.concatenate(hs, axis=0).T.astype(BF)
        for lo in range(0, dim, DC):
            cols = pl.ds(lo, DC)
            write(cols, jnp.dot(hbuf[pl.ds(0, m), pl.ds(0, n)], d_ref[:, cols], preferred_element_type=F32))

    def weigh():
        group, pair = 4 * rows, 2 * rows
        lane = lax.broadcasted_iota(jnp.int32, (8, pair), 1)
        for slot, offset in enumerate(OFFSETS):
            gz = lax.rem(z + offset + NZ, NZ)
            lanes = pl.ds(pl.multiple_of(gz * group, group), group)
            for j in range(4):
                expert = (z * 4 + xl * 2 + (c if j < 2 else 1 - c)) * 2 + j % 2
                row = jnp.sum(jnp.where(idv[:, lanes] == expert, prv[:, lanes], 0.0), axis=0, keepdims=True)
                lo, hi = (jnp.broadcast_to(row[:, at : at + pair], (8, pair)) for at in (0, pair))
                even = jnp.where(lane < rows, lo, pltpu.roll(hi, rows, 1))
                odd = jnp.where(lane < rows, pltpu.roll(lo, rows, 1), hi)
                wsc[j : j + 1, slot * pair : (slot + 1) * pair] = jnp.where(c == 0, even, odd)[0:1]

    def compute(k):
        ss = slots(k)
        s0, ns = ss[0], len(ss)
        pair = 2 * rows
        scales = [wsc[j : j + 1, s0 * pair : (s0 + ns) * pair] for j in range(4)]

        def write(cols, p):
            part[pl.ds(s0, ns), :, :, cols] = p.astype(BF).reshape(ns, 2, rows, DC)

        ffn(gath[pl.ds(s0, ns)].reshape(ns * pair, dim), wguv, wdv, scales, write)
        if k == 0:
            part[0, xl] = (part[0, xl].astype(F32) + sbuf[...]).astype(BF)

    sides = ((0, xup), (1, xdn))

    def x_send(slot, h, dev, which):
        r, cols = pl.ds(h * half, half), bounds[which]
        send(
            f"xx{which}", part.at[slot, other, r, cols], xx.at[slot, r, cols],
            xx_sem.at[slot, h, which], dev,
        )

    bounds = (pl.ds(0, cr), pl.ds(cr, sr))

    def swap_y(k):
        for slot in slots(k):
            for i in range(1, NY):
                send(
                    "yy", part.at[slot, :, :, pl.ds(cr + i * sr, sr)], yy.at[slot, NY - i - 1],
                    yr_sem.at[slot], {"y": yat[i]},
                )
        swap_common(k, True)

    def swap_common(k, soon):
        for slot in slots(k):
            for h, dev in sides:
                if soon == (k in (0, 4) or (h == 0) == (OFFSETS[slot] < 0)):
                    x_send(slot, h, dev, 0)

    def swap_late(k):
        swap_common(k, False)

    def sliced(slot, b, r):
        v = part[slot, b, r, cr:rw].astype(F32)
        for i in range(NY - 1):
            v = v + yy[slot, i, b, r].astype(F32)
        return v

    def swap_x(k):
        for slot in slots(k):
            arrive(yy.at[slot], yr_sem.at[slot])
            part[slot, other, :, cr:rw] = sliced(slot, other, slice(None)).astype(BF)
            for h, dev in sides:
                x_send(slot, h, dev, 1)

    def ring_step(s, which, cols, r_in, r_full, sem, h, up):
        slot = SLOT[(-s if up else s) % NZ]
        v = xx[slot, r_full, cols].astype(F32)
        v = v + (sliced(slot, xl, r_full) if which else part[slot, xl, r_full, cols].astype(F32))
        if s > 1:
            arrive(zin.at[h, s - 2, r_in, cols], sem(s - 2))
            v = v + zin[h, s - 2, r_in, cols].astype(F32)
        if s == NZ:
            return v.astype(BF)
        zout[h, s - 1, r_in, cols] = v.astype(BF)
        send(
            f"zz{which}", zout.at[h, s - 1, r_in, cols], zin.at[h, s - 1, r_in, cols],
            sem(s - 1), zup if up else zdn,
        )

    directions = ((0, True), (1, False))

    def ring(s):
        for h, up in directions:
            slot = SLOT[(-s if up else s) % NZ]
            x_at = xx.at[slot, pl.ds(h * half, half), bounds[0]]
            arrive(x_at, xx_sem.at[slot, h, 0])
        n = cr // NP
        for q, p in [(q, p) for q in (0, 1) for p in range(NP)]:
            for h, up in directions:
                v = ring_step(
                    s, 0, pl.ds(p * n, n), pl.ds(q * quarter, quarter),
                    pl.ds(h * half + q * quarter, quarter),
                    lambda i: zin_sem.at[h, i, q * NP + p], h, up,
                )
                for i in range(NY // NP if s == NZ else 0):
                    at = 2 * (p * NY // NP + i) + h
                    tsb[at, q * quarter : (q + 1) * quarter, 0:cw] = v[:, i * cw : (i + 1) * cw]

    def ring_slice(s):
        for h, up in directions:
            slot = SLOT[(-s if up else s) % NZ]
            full = pl.ds(h * half, half)
            arrive(xx.at[slot, full, bounds[1]], xx_sem.at[slot, h, 1])
            v = ring_step(s, 1, bounds[1], pl.ds(0, half), full, lambda i: zin_sem.at[h, i, 2 * NP], h, up)
            if s == NZ:
                tsb[2 * y + h, :, cw : cw + sr] = v

    cw = cr // NY

    def tensor_send(far):
        n = cw if far else cw + sr
        for yp, xp, i, j in peers:
            if far == min(i, 1):
                send(
                    f"t{far}", tsb.at[2 * yp + xp, :, pl.ds(0, n)],
                    tsi.at[2 * ((NY - i) % NY) + j, :, pl.ds(0, n)],
                    ts_sem.at[far], {"y": yp, "xh": xp},
                )

    for cp in tok_cp:
        cp.wait()
    for h in (0, 1):
        hop(0, h, True)
        hop(0, h, False)
        across(0, h)
    for cp in rt_cp:
        cp.wait()
    moved = ((wguv, 2 * hid), (wdv, hid))
    for i, (ref, n) in enumerate(moved):
        send(f"w{i}", ref.at[pl.ds(0, n)], ref.at[pl.ds(n, n)], wt_sem.at[i], mate)
    for cp in id_cp + sh_cp:
        cp.wait()

    def write_shared(cols, p):
        sbuf[:, cols] = p

    with jax.named_scope("shared"):
        ffn(gath[0, xl], sguv, sdv, None, write_shared)
    with jax.named_scope("weigh"):
        weigh()

    def weights():
        for i, (ref, n) in enumerate(moved):
            arrive(ref.at[pl.ds(n, n)], wt_sem.at[i])

    with jax.named_scope("s00_gz1"):
        gather_z(1)
    with jax.named_scope("s01_gx0"):
        gather_x(0)
    with jax.named_scope("s02_gz2"):
        gather_z(2)
    with jax.named_scope("s03_gx1"):
        gather_x(1)
    with jax.named_scope("s04_gy0"):
        gather_y(0)
    with jax.named_scope("s05_w"):
        weights()
    with jax.named_scope("s06_c0"):
        compute(0)
    with jax.named_scope("s07_gz3"):
        gather_z(3)
    with jax.named_scope("s08_gx2"):
        gather_x(2)
    with jax.named_scope("s09_gy1"):
        gather_y(1)
    with jax.named_scope("s10_c1"):
        compute(1)
    with jax.named_scope("s11_gz4"):
        gather_z(4)
    with jax.named_scope("s12_sy1"):
        swap_y(1)
    with jax.named_scope("s13_gx3"):
        gather_x(3)
    with jax.named_scope("s14_gy2"):
        gather_y(2)
    with jax.named_scope("s15_c2"):
        compute(2)
    with jax.named_scope("s16_sy2"):
        swap_y(2)
    with jax.named_scope("s17_sx1"):
        swap_x(1)
    with jax.named_scope("s18_gx4"):
        gather_x(4)
    with jax.named_scope("s19_r1"):
        ring(1)
    with jax.named_scope("s20_gy3"):
        gather_y(3)
    with jax.named_scope("s21_c3"):
        compute(3)
    with jax.named_scope("s22_sy3"):
        swap_y(3)
    with jax.named_scope("s23_sx2"):
        swap_x(2)
    with jax.named_scope("s24_gy4"):
        gather_y(4)
    with jax.named_scope("s25_r2"):
        ring(2)
    with jax.named_scope("s26_q1"):
        ring_slice(1)
    with jax.named_scope("s27_c4"):
        compute(4)
    with jax.named_scope("s28_sy4"):
        swap_y(4)
    with jax.named_scope("s29_sx3"):
        swap_x(3)
    with jax.named_scope("s30_r3"):
        ring(3)
    with jax.named_scope("s31_q2"):
        ring_slice(2)
    with jax.named_scope("s32_xl3"):
        swap_late(3)
    with jax.named_scope("s33_sx4"):
        swap_x(4)
    with jax.named_scope("s34_r4"):
        ring(4)
    with jax.named_scope("s35_q3"):
        ring_slice(3)
    with jax.named_scope("s36_xl2"):
        swap_late(2)
    with jax.named_scope("s37_r5"):
        ring(5)
    with jax.named_scope("s38_q4"):
        ring_slice(4)
    with jax.named_scope("s39_xl1"):
        swap_late(1)
    with jax.named_scope("s40_sy0"):
        swap_y(0)
    with jax.named_scope("s41_r6"):
        ring(6)
    with jax.named_scope("s42_q5"):
        ring_slice(5)
    with jax.named_scope("s43_sx0"):
        swap_x(0)
    with jax.named_scope("s44_r7"):
        ring(7)
    with jax.named_scope("s45_q6"):
        ring_slice(6)
    with jax.named_scope("s46_q7"):
        ring_slice(7)
    with jax.named_scope("s47_r8"):
        ring(8)
    with jax.named_scope("s48_t"):
        tensor_send(1)
    with jax.named_scope("s49_q8"):
        ring_slice(8)
    me = 2 * y + xh
    with jax.named_scope("tensor_sum"):
        tensor_send(0)
        mate_sum, far_sums = tsi.at[1, :, pl.ds(0, cw + sr)], tsi.at[pl.ds(2, 6), :, pl.ds(0, cw)]
        arrive(mate_sum, ts_sem.at[0])
        acc = tsb[me, :, 0:cw].astype(F32) + tsi[1, :, 0:cw].astype(F32)
        fin[:, cw : cw + sr] = (
            tsb[me, :, cw : cw + sr].astype(F32) + tsi[1, :, cw : cw + sr].astype(F32)
        ).astype(BF)
        arrive(far_sums, ts_sem.at[1])
        for i in range(2, 8):
            acc = acc + tsi[i, :, 0:cw].astype(F32)
        fin[:, 0:cw] = acc.astype(BF)
    with jax.named_scope("tensor_all"):
        for yp, xp, i, j in peers:
            send("t2", fin, agi.at[me], ta_sem.at[0], {"y": yp, "xh": xp})
        agi[me] = fin[...]
        others = agi.at[pl.ds(0, 7)]
        arrive(others, ta_sem.at[0])
        for i in range(NY):
            for j in (0, 1):
                r = pl.ds(j * half, half)
                out[r, i * cw : (i + 1) * cw] = agi[2 * i + j, :, 0:cw]
                out[r, cr + i * sr : cr + (i + 1) * sr] = agi[2 * i + j, :, cw : cw + sr]
    all_sent("z", gath.at[pl.ds(0, 7), 0, :, pl.ds(0, aw)])
    all_sent("x", gath.at[:, 0, :, pl.ds(0, aw)])
    if GA:
        all_sent("y", gath.at[pl.ds(0, 7), :, :, pl.ds(0, 3 * sa)])
        all_sent("y0", gath.at[0, 0, :, pl.ds(0, 3 * sa)])
    all_sent("xx0", part.at[:, 0, :, pl.ds(0, cr)])
    all_sent("xx1", part.at[:, 0, :, pl.ds(0, sr)])
    all_sent("yy", yy)
    all_sent("zz0", zout.at[:, :, :, bounds[0]])
    all_sent("zz1", zout.at[:, :, :, bounds[1]])
    for i, (ref, n) in enumerate(moved):
        all_sent(f"w{i}", ref.at[pl.ds(0, n)])
    all_sent("t0", mate_sum)
    all_sent("t1", far_sums)
    all_sent("t2", others)


def layer(tokens, ids, probs, wg, wu, wd, sg, su, sd):
    rows, dim = tokens.shape
    hid = sg.shape[0]
    rw = dim - GR + GR // NY
    any_spec = pl.BlockSpec(memory_space=pl.ANY)
    dma = pltpu.SemaphoreType.DMA
    last = (2 * NY, rows // 2, dim // NY)
    return pl.pallas_call(
        kernel,
        out_shape=jax.ShapeDtypeStruct((rows, dim), BF),
        in_specs=[any_spec] * 9,
        out_specs=pl.BlockSpec(memory_space=pltpu.VMEM),
        scratch_shapes=[
            pltpu.VMEM((NZ, 2, rows, dim), BF),
            pltpu.VMEM((NZ, 2, rows, dim), BF),
            pltpu.VMEM((NZ, NY - 1, 2, rows, max(GR // NY, 128)), BF),
            pltpu.VMEM((NZ, rows, rw), BF),
            pltpu.VMEM((2, NZ - 1, rows // 2, rw), BF),
            pltpu.VMEM((2, NZ - 1, rows // 2, rw), BF),
            pltpu.VMEM((4 * hid, dim), BF),
            pltpu.VMEM((2 * hid, dim), BF),
            pltpu.VMEM((2 * hid, dim), BF),
            pltpu.VMEM((hid, dim), BF),
            pltpu.VMEM(ids.shape, jnp.int32),
            pltpu.VMEM(probs.shape, F32),
            pltpu.VMEM((8, NZ * 2 * rows), F32),
            pltpu.VMEM((4 * rows, 2 * hid), BF),
            pltpu.VMEM((rows, dim), F32),
            pltpu.VMEM(last, BF),
            pltpu.VMEM(last, BF),
            pltpu.VMEM(last[1:], BF),
            pltpu.VMEM(last, BF),
            dma((9,)), dma((15,)), dma((2,)), dma((NZ, 2)), dma((NZ,)), dma((NZ,)),
            dma((NZ,)), dma((NZ, 2, 2)), dma((2, NZ - 1, 2 * NP + 1)), dma((2,)), dma((1,)),
        ],
        compiler_params=pltpu.CompilerParams(
            collective_id=0, has_side_effects=True, vmem_limit_bytes=62 * 1024 * 1024
        ),
    )(tokens, ids, probs, wg, wu, wd, sg, su, sd)


def body(tokens, expert_ids, gate_probs, w_gate, w_up, w_down, shared_gate, shared_up, shared_down):
    dim = tokens.shape[1]
    stacked = lambda w: jnp.swapaxes(w, 1, 2).reshape(-1, dim)
    return layer(
        tokens, expert_ids.T, gate_probs.T, stacked(w_gate), stacked(w_up), w_down.reshape(-1, dim),
        shared_gate.T, shared_up.T, shared_down,
    )


def solution(mesh):
    torus = Mesh(mesh.devices.reshape(NZ, 2, 2, 4, 2), ("z", "xl", "c", "y", "xh"))
    e, t = ("z", "xl", "c"), ("y", "xh")
    return jax.shard_map(
        body,
        mesh=torus,
        in_specs=(
            P(e, None), P(), P(),
            P(e, None, t), P(e, None, t), P(e, t, None),
            P(None, t), P(None, t), P(t, None),
        ),
        out_specs=P(e, None),
        check_vma=False,
    )
```
